32 devices in a mesh: dp: 8 (over z, x), tensor: 4 (over y, core).
Axes of the slice: x: 2, y: 2, z: 4, core: 2. Of those that a mesh axis runs over, the one named last changes fastest.
Arguments:
- widened_in: bfloat16 [16384, 1536], P(('dp', 'tensor')), may hold values from -6 to 6
- encoder_states: bfloat16 [4096, 768], P(('dp', 'tensor')), may hold values from -6 to 6
- predict: float32 [2, 2], replicated, may hold values from 0.25 to 1.25
- correct_gain: float32 [2], replicated, may hold values from 0.5 to 1.5
- self_gain: float32 [768], replicated, may hold values from 0.1 to 1.9
- self_q: bfloat16 [768, 768], P('dp', 'tensor'), may hold values from -0.21875 to 0.21875
- self_k: bfloat16 [768, 768], P('dp', 'tensor'), may hold values from -0.21875 to 0.21875
- self_v: bfloat16 [768, 768], P('dp', 'tensor'), may hold values from -0.21875 to 0.21875
- self_o: bfloat16 [768, 768], P('dp', 'tensor'), may hold values from -1.75 to 1.75
- cross_gain: float32 [768], replicated, may hold values from 0.1 to 1.9
- cross_q: bfloat16 [768, 768], P('dp', 'tensor'), may hold values from -0.21875 to 0.21875
- cross_k: bfloat16 [768, 768], P('dp', 'tensor'), may hold values from -0.21875 to 0.21875
- cross_v: bfloat16 [768, 768], P('dp', 'tensor'), may hold values from -0.21875 to 0.21875
- cross_o: bfloat16 [768, 768], P('dp', 'tensor'), may hold values from -1.75 to 1.75
- ffn_gain: float32 [768], replicated, may hold values from 0.1 to 1.9
- ffn_gate: bfloat16 [768, 3072], P('dp', 'tensor'), may hold values from -0.21875 to 0.21875
- ffn_up: bfloat16 [768, 3072], P('dp', 'tensor'), may hold values from -0.21875 to 0.21875
- ffn_down: bfloat16 [768, 3072], P('dp', 'tensor'), may hold values from -0.109375 to 0.109375
- segment_ids: int32 [8, 2048], P('dp'), may hold values from 0 to 5, never falling along the last dimension, each value on 1 to 819 neighbouring positions
- encoder_ids: int32 [8, 512], P('dp'), may hold values from 0 to 5, never falling along the last dimension, each value on 1 to 204 neighbouring positions
- block_choice: int32 [16384], P(('dp', 'tensor')), may hold values from 0 to 1
- out_grad: bfloat16 [16384, 1536], P(('dp', 'tensor')), may hold values from -6 to 6
Outputs:
- widened_out: bfloat16 [16384, 1536], P(('dp', 'tensor'))
- input_grad: float32 [16384, 1536], P(('dp', 'tensor'))
- encoder_grad: float32 [4096, 768], P(('dp', 'tensor'))
- predict_grad: float32 [2, 2], replicated
- correct_gain_grad: float32 [2], replicated
- self_gain_grad: float32 [768], replicated
- self_q_grad: float32 [768, 768], P('dp', 'tensor')
- self_k_grad: float32 [768, 768], P('dp', 'tensor')
- self_v_grad: float32 [768, 768], P('dp', 'tensor')
- self_o_grad: float32 [768, 768], P('dp', 'tensor')
- cross_gain_grad: float32 [768], replicated
- cross_q_grad: float32 [768, 768], P('dp', 'tensor')
- cross_k_grad: float32 [768, 768], P('dp', 'tensor')
- cross_v_grad: float32 [768, 768], P('dp', 'tensor')
- cross_o_grad: float32 [768, 768], P('dp', 'tensor')
- ffn_gain_grad: float32 [768], replicated
- ffn_gate_grad: float32 [768, 3072], P('dp', 'tensor')
- ffn_up_grad: float32 [768, 3072], P('dp', 'tensor')
- ffn_down_grad: float32 [768, 3072], P('dp', 'tensor')
The draws below stay inside these ranges and needn't reach their ends.
Inputs may be any that keep to these rules, and one draw needn't show every extreme that they name: `segment_ids`: each sequence holds 6 documents numbered in order; the longest has exactly 819 tokens. `encoder_ids`: each of a sequence's 6 document numbers appears among its encoder states, in order; the longest has exactly 204 states.
All inputs are finite; a program needn't handle non-finite values.
Results may differ from the reference program's by a relative error of at most 0.025.
Values may be sent and summed in bfloat16 or wider, within the bound.
A program may use at most 192 MiB of HBM per device.

```python
import math
import jax
import jax.numpy as jnp
import numpy as np
from jax import lax

D = 768
HEADS = 12
HDIM = 64
FF = 3072
SEQ = 2048
ENC = 512
DOCS = 6
SEQS = 8
TOKENS = 16384
ENC_ROWS = 4096
HD_ALL = 768
DOC_MOST = 819
ENC_MOST = 204


def with_ends(values, rng, low, high):
    index_at = [jax.random.randint(jax.random.fold_in(rng, axis), (), 0, length) for axis, length in enumerate(values.shape)]
    main_axis = values.shape.index(max(values.shape))
    next_to = index_at[:main_axis] + [(index_at[main_axis] + 1) % values.shape[main_axis]] + index_at[main_axis + 1:]
    return values.at[tuple(index_at)].set(low).at[tuple(next_to)].set(high)


def shard_levels(stream_key, dims, pieces, smallest, high):
    def one(position, blocks):
        steps = jax.random.uniform(jax.random.fold_in(jax.random.fold_in(stream_key, 6), position), (blocks,), jnp.float32, smallest / len(pieces), high / len(pieces))
        return jnp.repeat(jnp.exp(steps), dims[position] // blocks).reshape((-1,) + (1,) * (len(dims) - position - 1))

    gain = one(*pieces[0])
    for cut in pieces[1:]:
        gain = gain * one(*cut)
    return gain


def profile(number_of, total, reach, slope):
    loads = [(1 << 20) // math.isqrt(grade ** slope) + 1 for grade in range(2, number_of + 1)]
    surplus, holding = total - reach - (number_of - 1), [1] * (number_of - 1)
    while surplus > 0:
        free = [i for i in range(number_of - 1) if holding[i] < reach]
        mass, budget = sum([loads[i] for i in free]), surplus
        for i in free:
            addition = min(reach - holding[i], max(1, budget * loads[i] // mass), surplus)
            holding[i] = holding[i] + addition
            surplus = surplus - addition
    return np.array([reach] + holding)


def ragged(key, amount, total, reach, skew):
    if amount == 2:
        one = jax.random.randint(key, (), max(1, total - reach), min(reach, total - 1) + 1)
        return jnp.stack([one, total - one])
    lengths = jnp.asarray(profile(amount, total, reach, skew), jnp.int32)
    couples = (amount - 1) // 2
    giver, sink = lengths[1:1 + 2 * couples:2], lengths[2:2 + 2 * couples:2]
    margin = jnp.minimum(giver - 1, reach - sink)
    passed = jax.random.randint(jax.random.fold_in(key, 1), (couples,), 0, 1 << 20) % (margin + 1)
    lengths = lengths.at[1:1 + 2 * couples:2].set(giver - passed).at[2:2 + 2 * couples:2].set(sink + passed)
    return lengths[jax.random.permutation(jax.random.fold_in(key, 2), amount)]


def normal_values(rng, shape, width, reach, cuts=(), kind=jnp.bfloat16):
    values = width * jax.random.normal(rng, shape, jnp.float32)
    if cuts:
        values = values * shard_levels(rng, shape, cuts, -0.22, 0.18)
    return jnp.clip(values, -reach, reach).astype(kind)


def setup_inputs(seed: int = 0) -> dict:
    key_list = jax.random.split(jax.random.key(seed), 23)
    widened_in = normal_values(key_list[0], (TOKENS, 2 * D), 1.0, 6.0, ((0, 32),))
    encoder_states = normal_values(key_list[1], (ENC_ROWS, D), 1.0, 6.0, ((0, 32),))
    predict = jnp.clip(jax.random.uniform(key_list[2], (2, 2), jnp.float32, 0.25, 1.25), 0.25, 1.25)
    correct_gain = jnp.clip(jax.random.uniform(key_list[3], (2,), jnp.float32, 0.5, 1.5), 0.5, 1.5)
    self_gain = jnp.clip(1.0 + 0.18 * jax.random.normal(key_list[4], (D,), jnp.float32), 0.1, 1.9)
    self_q = normal_values(key_list[5], (D, HD_ALL), D ** -0.5, 0.21875, ((0, 8), (1, 4)))
    self_k = normal_values(key_list[6], (D, HD_ALL), D ** -0.5, 0.21875, ((0, 8), (1, 4)))
    self_v = normal_values(key_list[7], (D, HD_ALL), D ** -0.5, 0.21875, ((0, 8), (1, 4)))
    self_o = normal_values(key_list[8], (D, HD_ALL), (max(HD_ALL // 64, 1)) ** -0.5, 1.75, ((0, 8), (1, 4)))
    cross_gain = jnp.clip(1.0 + 0.18 * jax.random.normal(key_list[9], (D,), jnp.float32), 0.1, 1.9)
    cross_q = normal_values(key_list[10], (D, HD_ALL), D ** -0.5, 0.21875, ((0, 8), (1, 4)))
    cross_k = normal_values(key_list[11], (D, HD_ALL), D ** -0.5, 0.21875, ((0, 8), (1, 4)))
    cross_v = normal_values(key_list[12], (D, HD_ALL), D ** -0.5, 0.21875, ((0, 8), (1, 4)))
    cross_o = normal_values(key_list[13], (D, HD_ALL), (max(HD_ALL // 64, 1)) ** -0.5, 1.75, ((0, 8), (1, 4)))
    ffn_gain = jnp.clip(1.0 + 0.18 * jax.random.normal(key_list[14], (D,), jnp.float32), 0.1, 1.9)
    ffn_gate = normal_values(key_list[15], (D, FF), D ** -0.5, 0.21875, ((0, 8), (1, 4)))
    ffn_up = normal_values(key_list[16], (D, FF), D ** -0.5, 0.21875, ((0, 8), (1, 4)))
    ffn_down = normal_values(key_list[17], (D, FF), FF ** -0.5, 0.109375, ((0, 8), (1, 4)))
    segment_ids = jax.vmap(lambda own: jnp.searchsorted(jnp.cumsum(ragged(own, DOCS, SEQ, DOC_MOST, 2)), jnp.arange(SEQ), side="right"))(jax.random.split(key_list[18], SEQS)).reshape((SEQS, SEQ)).astype(jnp.int32)
    encoder_ids = jax.vmap(lambda own: jnp.searchsorted(jnp.cumsum(ragged(own, DOCS, ENC, ENC_MOST, 2)), jnp.arange(ENC), side="right"))(jax.random.split(key_list[19], SEQS)).reshape((SEQS, ENC)).astype(jnp.int32)
    block_choice = with_ends(jax.random.randint(key_list[20], (TOKENS,), 0, 2), jax.random.fold_in(key_list[20], 1), 0, 1).astype(jnp.int32)
    out_grad = normal_values(key_list[21], (TOKENS, 2 * D), 1.0, 6.0, ((0, 32),))
    return {"widened_in": widened_in, "encoder_states": encoder_states, "predict": predict, "correct_gain": correct_gain, "self_gain": self_gain, "self_q": self_q, "self_k": self_k, "self_v": self_v, "self_o": self_o, "cross_gain": cross_gain, "cross_q": cross_q, "cross_k": cross_k, "cross_v": cross_v, "cross_o": cross_o, "ffn_gain": ffn_gain, "ffn_gate": ffn_gate, "ffn_up": ffn_up, "ffn_down": ffn_down, "segment_ids": segment_ids, "encoder_ids": encoder_ids, "block_choice": block_choice, "out_grad": out_grad}


@jax.custom_vjp
def low(v):
    return lax.optimization_barrier(v.astype(jnp.bfloat16)).astype(jnp.float32)

@jax.custom_vjp
def low_back(v):
    return v

def low_keep(v):
    return (low(v), None)

def low_pass(kept, grad):
    return (grad,)

def back_keep(v):
    return (v, None)

def back_low(kept, grad):
    return (low(grad),)
low.defvjp(low_keep, low_pass)
low_back.defvjp(back_keep, back_low)
highest = lax.Precision.HIGHEST

def matmul(left_mat, right_mat):
    return jnp.dot(left_mat, right_mat, precision=highest, preferred_element_type=jnp.float32)

def both_ways(values):
    return low_back(low(values))

def rms_norm(values, norm_gain):
    return values * lax.rsqrt(lax.optimization_barrier(jnp.mean(values * values, axis=-1, keepdims=True)) + 1e-06) * norm_gain

def build_mask(query_ids, key_ids, row_start, causal):
    allowed = query_ids[:, None] == key_ids[None, :]
    if causal:
        rows_at = row_start + jnp.arange(query_ids.shape[0], dtype=jnp.int32)
        cols_at = jnp.arange(key_ids.shape[0], dtype=jnp.int32)
        allowed = jnp.logical_and(allowed, cols_at[None, :] <= rows_at[:, None])
    return allowed

def attend_sequence(queries, key_rows, value_rows, query_ids, key_ids, causal):
    total_rows = queries.shape[0]
    block_rows = min(512, total_rows)
    block_count = total_rows // block_rows
    q_pieces = queries.reshape(block_count, block_rows, HEADS, HDIM)
    id_pieces = query_ids.reshape(block_count, block_rows)
    starts = jnp.arange(block_count, dtype=jnp.int32) * block_rows
    shaped_keys = key_rows.reshape(-1, HEADS, HDIM)
    shaped_values = value_rows.reshape(-1, HEADS, HDIM)

    def attend_one(members):
        q_piece, ids_here, row_start = members
        allowed = build_mask(ids_here, key_ids, row_start, causal)[None]
        scores = low_back(jnp.einsum('qhd,khd->hqk', q_piece, shaped_keys, precision=highest) * HDIM ** (-0.5))
        masked = jnp.where(allowed, scores, -1e+30)
        row_max = lax.optimization_barrier(jnp.max(masked, axis=-1, keepdims=True))
        weights = jnp.where(allowed, jnp.exp(masked - row_max), 0.0)
        attn_probs = low(weights / lax.optimization_barrier(jnp.sum(weights, axis=-1, keepdims=True)))
        return jnp.einsum('hqk,khd->qhd', attn_probs, shaped_values, precision=highest)
    mixed_rows = lax.map(jax.checkpoint(attend_one), (q_pieces, id_pieces, starts))
    return mixed_rows.reshape(total_rows, HEADS * HDIM)

def attend_all(queries, key_rows, value_rows, query_ids, key_ids, causal):
    seq_count = query_ids.shape[0]

    def per_sequence(members):
        seq_q, seq_k, seq_v, seq_qid, seq_kid = members
        return attend_sequence(seq_q, seq_k, seq_v, seq_qid, seq_kid, causal)
    mixed_rows = lax.map(per_sequence, (queries.reshape(seq_count, -1, HEADS * HDIM), key_rows.reshape(seq_count, -1, HEADS * HDIM), value_rows.reshape(seq_count, -1, HEADS * HDIM), query_ids, key_ids))
    return mixed_rows.reshape(-1, HEADS * HDIM)

def decoder_forward(widened, encoder, predict, correct_gain, self_gain, self_q, self_k, self_v, self_o, cross_gain, cross_q, cross_k, cross_v, cross_o, ffn_gain, ffn_gate, ffn_up, ffn_down, segment_ids, encoder_ids, block_choice):
    half_width = widened.shape[1] // 2
    first_block = widened[:, :half_width]
    second_block = widened[:, half_width:]
    pred_first = predict[0, 0] * first_block + predict[0, 1] * second_block
    pred_second = predict[1, 0] * first_block + predict[1, 1] * second_block
    picked = (block_choice == 1)[:, None]
    chosen = jnp.where(picked, second_block, first_block)
    pred_chosen = jnp.where(picked, pred_second, pred_first)
    normed_self = low(rms_norm(chosen, self_gain))
    self_query = both_ways(matmul(normed_self, self_q))
    self_key = both_ways(matmul(normed_self, self_k))
    self_value = both_ways(matmul(normed_self, self_v))
    self_mix = both_ways(attend_all(self_query, self_key, self_value, segment_ids, segment_ids, True))
    after_self = chosen + low_back(matmul(self_mix, self_o.T))
    normed_cross = low(rms_norm(after_self, cross_gain))
    cross_query = both_ways(matmul(normed_cross, cross_q))
    cross_key = both_ways(matmul(encoder, cross_k))
    cross_value = both_ways(matmul(encoder, cross_v))
    cross_mix = both_ways(attend_all(cross_query, cross_key, cross_value, segment_ids, encoder_ids, False))
    after_cross = after_self + low_back(matmul(cross_mix, cross_o.T))
    normed_ffn = low(rms_norm(after_cross, ffn_gain))
    gate = low_back(matmul(normed_ffn, ffn_gate))
    up_rows = low_back(matmul(normed_ffn, ffn_up))
    hidden = low(jax.nn.gelu(gate, approximate=True) * up_rows)
    computed = after_cross + low_back(matmul(hidden, ffn_down.T))
    gap = computed - pred_chosen
    return jnp.concatenate([pred_first + correct_gain[0] * gap, pred_second + correct_gain[1] * gap], axis=1)

def reference(widened_in, encoder_states, predict, correct_gain, self_gain, self_q, self_k, self_v, self_o, cross_gain, cross_q, cross_k, cross_v, cross_o, ffn_gain, ffn_gate, ffn_up, ffn_down, segment_ids, encoder_ids, block_choice, out_grad):
    floats = (widened_in.astype(jnp.float32), encoder_states.astype(jnp.float32), predict, correct_gain, self_gain, self_q.astype(jnp.float32), self_k.astype(jnp.float32), self_v.astype(jnp.float32), self_o.astype(jnp.float32), cross_gain, cross_q.astype(jnp.float32), cross_k.astype(jnp.float32), cross_v.astype(jnp.float32), cross_o.astype(jnp.float32), ffn_gain, ffn_gate.astype(jnp.float32), ffn_up.astype(jnp.float32), ffn_down.astype(jnp.float32))

    def forward(*params):
        return decoder_forward(*params, segment_ids, encoder_ids, block_choice)
    output, pullback = jax.vjp(forward, *floats)
    grads = pullback(out_grad.astype(jnp.float32))
    return (output.astype(jnp.bfloat16), grads[0], grads[1], grads[2], grads[3], grads[4], grads[5], grads[6], grads[7], grads[8], grads[9], grads[10], grads[11], grads[12], grads[13], grads[14], grads[15], grads[16], grads[17])
```

```python
import functools
import jax
import jax.numpy as jnp
from jax import lax
from jax.experimental import pallas as pl
from jax.experimental.pallas import tpu as pltpu
from jax.sharding import Mesh, PartitionSpec as P

HDIM = 64
DOCS = 6
epsilon = 1e-06
f32 = jnp.float32
bf16 = jnp.bfloat16
NEG = -1e30
Q_TILE = 256


def tdot(left_mat, right_mat):
    return lax.dot_general(
        left_mat, right_mat, (((0,), (0,)), ((), ())), preferred_element_type=f32
    )


def ndot(left_mat, right_mat):
    return lax.dot_general(
        left_mat, right_mat, (((1,), (1,)), ((), ())), preferred_element_type=f32
    )


def mdot(left_mat, right_mat):
    return jnp.dot(left_mat, right_mat, preferred_element_type=f32)


def rms_forward(values, norm_gain):
    factor = lax.rsqrt(jnp.mean(values * values, axis=-1, keepdims=True) + epsilon)
    return values * factor * norm_gain


def rms_backward(values, norm_gain, d_normed):
    factor = lax.rsqrt(jnp.mean(values * values, axis=-1, keepdims=True) + epsilon)
    scaled = d_normed * norm_gain
    d_values = factor * scaled - values * factor * factor * factor * jnp.mean(
        scaled * values, axis=-1, keepdims=True
    )
    gain_grad = jnp.sum(d_normed * values * factor, axis=0)
    return (d_values, gain_grad)


def swap_core(rows):
    return lax.ppermute(rows, "core", [(0, 1), (1, 0)])


def swap_ty(rows):
    return lax.ppermute(rows, "ty", [(0, 1), (1, 0)])


def swap_bit(rows, bit):
    size = lax.axis_size("dp")
    return lax.ppermute(rows, "dp", [(i, i ^ (1 << bit)) for i in range(size)])


def my_bit(bit):
    return (lax.axis_index("dp") >> bit) & 1


def dp_bits():
    return lax.axis_size("dp").bit_length() - 1


def grow(piece, bit, have):
    other = swap_bit(piece, bit)
    low = my_bit(bit) == 0
    at = sum(1 for known in have if known > bit)
    return jnp.stack([jnp.where(low, piece, other), jnp.where(low, other, piece)], axis=at)


def gather_weight(piece, y_last):
    rows, cols = piece.shape
    bits = dp_bits()
    have = []
    for bit in range(1, bits):
        piece = grow(piece, bit, have)
        have.append(bit)
    if y_last:
        piece = grow(piece, 0, have)
        slabs = [piece, swap_ty(piece)]
    else:
        slabs = [grow(slab, 0, have) for slab in (piece, swap_ty(piece))]
    return [slab.reshape(-1, cols) for slab in slabs]


def plus(left_mat, right_mat):
    return (left_mat.astype(f32) + right_mat.astype(f32)).astype(bf16)


def shrink(partial, bit, left):
    at = sum(1 for known in left if known > bit)
    mine = my_bit(bit)
    sent = lax.dynamic_index_in_dim(partial, 1 - mine, at, keepdims=False)
    kept = lax.dynamic_index_in_dim(partial, mine, at, keepdims=False)
    return plus(kept, swap_bit(sent, bit))


def reduce_weight(slabs, y_first):
    bits = dp_bits()
    size = lax.axis_size("dp")
    rows, cols = slabs[0].shape
    shaped = [s.reshape((2,) * bits + (rows // size, cols)) for s in slabs]
    left = list(range(bits))
    if y_first:
        total = plus(shaped[0], swap_ty(shaped[1]))
        total = shrink(total, 0, left)
    else:
        shaped = [shrink(s, 0, left) for s in shaped]
        total = plus(shaped[0], swap_ty(shaped[1]))
    left.remove(0)
    for bit in reversed(range(1, bits)):
        total = shrink(total, bit, left)
        left.remove(bit)
    return total.astype(f32)


def sum_everywhere(values):
    for bit in range(dp_bits()):
        values = values + swap_bit(values, bit)
    values = values + swap_ty(values)
    return values + swap_core(values)


def pair_rows(own_rows):
    return jnp.concatenate([own_rows, swap_core(own_rows)], axis=0)


def pair_sum(part, rows):
    sent = part(rows, 2 * rows).astype(bf16)
    arrived = swap_core(sent)
    return part(0, rows) + arrived.astype(f32)


def head_parts(block):
    lane = lax.broadcasted_iota(jnp.int32, (block.shape[0], 128), 1)
    pair = block[:, 0:128]
    zero = jnp.zeros_like(pair)
    return [
        jnp.where(lane < HDIM, pair, zero),
        jnp.where(lane < HDIM, zero, pair),
        block[:, 128:192],
    ]


LANES = ((0, 128), (0, 128), (128, 192))


def allowed_keys(key_base, tile, lo, hi):
    key_at = lax.broadcasted_iota(jnp.int32, (tile, lo.shape[1]), 0) + key_base
    return jnp.logical_and(key_at >= lo, key_at <= hi)


def forward_kernel(
    tile, table, q0, q1, k0, k1, v0, v1, lo_ref, hi_ref, mix0, mix1, lse_ref, acc, peak, total
):
    step = pl.program_id(0)
    lo, hi = lo_ref[...], hi_ref[...]
    acc[...] = jnp.zeros_like(acc)
    peak[...] = jnp.full_like(peak, NEG)
    total[...] = jnp.zeros_like(total)
    queries = [head_parts(q[...] * 0.125) for q in (q0, q1)]
    steps = pl.num_programs(0)

    def one(at, carry):
        off = pl.multiple_of(table[2 * steps + at], tile)
        allow = allowed_keys(at * tile, tile, lo, hi)
        for slab, (k_ref, v_ref) in enumerate(((k0, v0), (k1, v1))):
            for head in range(3):
                first, last = LANES[head]
                row = slab * 3 + head
                keys = k_ref[pl.ds(off, tile), first:last]
                values = v_ref[pl.ds(off, tile), first:last]
                scores = jnp.where(allow, ndot(keys, queries[slab][head]), NEG)
                old = peak[row : row + 1, :]
                top = jnp.maximum(old, jnp.max(scores, axis=0, keepdims=True))
                weights = jnp.exp(scores - top)
                fade = jnp.exp(old - top)
                total[row : row + 1, :] = total[row : row + 1, :] * fade + jnp.sum(
                    weights, axis=0, keepdims=True
                )
                peak[row : row + 1, :] = top
                fresh = tdot(values, weights.astype(bf16))
                if head == 1:
                    fresh = fresh[HDIM:, :]
                elif head == 0:
                    fresh = fresh[:HDIM, :]
                span = slice(row * HDIM, (row + 1) * HDIM)
                acc[span, :] = acc[span, :] * fade + fresh
        return carry

    lax.fori_loop(table[step], table[steps + step], one, 0)
    lse_ref[...] = peak[...] + jnp.log(total[...])
    for slab, mix in enumerate((mix0, mix1)):
        pieces = []
        for head in range(3):
            row = slab * 3 + head
            pieces.append(acc[row * HDIM : (row + 1) * HDIM, :] / total[row : row + 1, :])
        mix[...] = jnp.concatenate(pieces, axis=0).T.astype(bf16)


def backward_kernel(
    tile,
    table,
    q0,
    q1,
    g0,
    g1,
    mix0,
    mix1,
    k0,
    k1,
    v0,
    v1,
    lo_ref,
    hi_ref,
    lse_ref,
    dq0,
    dq1,
    dk0,
    dk1,
    dv0,
    dv1,
    acc,
    key_acc0,
    key_acc1,
    value_acc0,
    value_acc1,
):
    step = pl.program_id(0)
    steps = pl.num_programs(0)
    lo, hi = lo_ref[...], hi_ref[...]

    @pl.when(step == 0)
    def _():
        for ref in (key_acc0, key_acc1, value_acc0, value_acc1):
            ref[...] = jnp.zeros_like(ref)

    acc[...] = jnp.zeros_like(acc)
    queries = [head_parts(q[...] * 0.125) for q in (q0, q1)]
    grads = [head_parts(g[...]) for g in (g0, g1)]
    inner = []
    for g, mix in ((g0, mix0), (g1, mix1)):
        both = (g[...].astype(f32) * mix[...].astype(f32)).T
        for head in range(3):
            inner.append(
                jnp.sum(both[head * HDIM : (head + 1) * HDIM, :], axis=0, keepdims=True)
            )

    def one(at, carry):
        off = pl.multiple_of(table[2 * steps + at], tile)
        allow = allowed_keys(at * tile, tile, lo, hi)
        for slab, (k_ref, v_ref, ka, va) in enumerate(
            ((k0, v0, key_acc0, value_acc0), (k1, v1, key_acc1, value_acc1))
        ):
            for head in range(3):
                first, last = LANES[head]
                row = slab * 3 + head
                keys = k_ref[pl.ds(off, tile), first:last]
                values = v_ref[pl.ds(off, tile), first:last]
                query, grad = queries[slab][head], grads[slab][head]
                scores = ndot(keys, query) - lse_ref[row : row + 1, :]
                probs = jnp.exp(jnp.where(allow, scores, NEG))
                d_probs = ndot(values, grad)
                d_scores = (probs * (d_probs - inner[row])).astype(bf16)
                va[pl.ds(off, tile), first:last] += mdot(probs.astype(bf16), grad)
                ka[pl.ds(off, tile), first:last] += mdot(d_scores, query)
                fresh = tdot(keys, d_scores)
                if head == 1:
                    fresh = fresh[HDIM:, :]
                elif head == 0:
                    fresh = fresh[:HDIM, :]
                span = slice(row * HDIM, (row + 1) * HDIM)
                acc[span, :] += fresh
        return carry

    lax.fori_loop(table[step], table[steps + step], one, 0)
    for slab, dq in enumerate((dq0, dq1)):
        dq[...] = (acc[slab * 192 : (slab + 1) * 192, :] * 0.125).T.astype(bf16)

    @pl.when(step == steps - 1)
    def _():
        dk0[...] = key_acc0[...].astype(bf16)
        dk1[...] = key_acc1[...].astype(bf16)
        dv0[...] = value_acc0[...].astype(bf16)
        dv1[...] = value_acc1[...].astype(bf16)


def attention_forward(table, lo, hi, queries, keys, values, tile):
    rows, cols = queries[0].shape
    total_keys = keys[0].shape[0]
    steps = rows // Q_TILE
    row_block = pl.BlockSpec((Q_TILE, cols), lambda i, t: (i, 0))
    key_block = pl.BlockSpec((total_keys, cols), lambda i, t: (0, 0))
    lane_block = pl.BlockSpec((1, Q_TILE), lambda i, t: (0, i))
    lse_block = pl.BlockSpec((8, Q_TILE), lambda i, t: (0, i))
    work = rows * total_keys * 2 * cols
    return pl.pallas_call(
        functools.partial(forward_kernel, tile),
        out_shape=(
            jax.ShapeDtypeStruct((rows, cols), bf16),
            jax.ShapeDtypeStruct((rows, cols), bf16),
            jax.ShapeDtypeStruct((8, rows), f32),
        ),
        grid_spec=pltpu.PrefetchScalarGridSpec(
            num_scalar_prefetch=1,
            grid=(steps,),
            in_specs=[row_block] * 2 + [key_block] * 4 + [lane_block] * 2,
            out_specs=(row_block, row_block, lse_block),
            scratch_shapes=[
                pltpu.VMEM((2 * cols, Q_TILE), f32),
                pltpu.VMEM((8, Q_TILE), f32),
                pltpu.VMEM((8, Q_TILE), f32),
            ],
        ),
        compiler_params=pltpu.CompilerParams(
            dimension_semantics=("arbitrary",), vmem_limit_bytes=32 << 20
        ),
        cost_estimate=pl.CostEstimate(
            flops=4 * work, bytes_accessed=8 * total_keys * cols, transcendentals=work // 64
        ),
        name="attend_forward",
    )(table, *queries, *keys, *values, lo, hi)


def attention_backward(table, lo, hi, lse, queries, grads, mixes, keys, values, tile):
    rows, cols = queries[0].shape
    total_keys = keys[0].shape[0]
    steps = rows // Q_TILE
    row_block = pl.BlockSpec((Q_TILE, cols), lambda i, t: (i, 0))
    key_block = pl.BlockSpec((total_keys, cols), lambda i, t: (0, 0))
    lane_block = pl.BlockSpec((1, Q_TILE), lambda i, t: (0, i))
    lse_block = pl.BlockSpec((8, Q_TILE), lambda i, t: (0, i))
    row_shape = jax.ShapeDtypeStruct((rows, cols), bf16)
    key_shape = jax.ShapeDtypeStruct((total_keys, cols), bf16)
    work = rows * total_keys * 2 * cols
    out = pl.pallas_call(
        functools.partial(backward_kernel, tile),
        out_shape=(row_shape, row_shape, key_shape, key_shape, key_shape, key_shape),
        grid_spec=pltpu.PrefetchScalarGridSpec(
            num_scalar_prefetch=1,
            grid=(steps,),
            in_specs=[row_block] * 6 + [key_block] * 4 + [lane_block] * 2 + [lse_block],
            out_specs=(row_block, row_block) + (key_block,) * 4,
            scratch_shapes=[pltpu.VMEM((2 * cols, Q_TILE), f32)]
            + [pltpu.VMEM((total_keys, cols), f32)] * 4,
        ),
        compiler_params=pltpu.CompilerParams(
            dimension_semantics=("arbitrary",), vmem_limit_bytes=48 << 20
        ),
        cost_estimate=pl.CostEstimate(
            flops=10 * work, bytes_accessed=16 * total_keys * cols, transcendentals=work // 64
        ),
        name="attend_backward",
    )(table, *queries, *grads, *mixes, *keys, *values, lo, hi, lse)
    return out[0:2], out[2:4], out[4:6]


def pick(ids, counts):
    out = jnp.zeros(ids.shape, jnp.int32)
    for doc in range(DOCS):
        out = jnp.where(ids == doc, counts[doc], out)
    return out


def key_tables(segment_ids, encoder_ids, rows, self_tile, cross_tile):
    chip, core = lax.axis_index("ty"), lax.axis_index("core")
    ids = segment_ids.reshape(-1)
    states = encoder_ids.reshape(-1)
    docs = jnp.arange(DOCS, dtype=jnp.int32)
    starts = jnp.sum(ids[None, :] < docs[:, None], axis=1, dtype=jnp.int32)
    state_first = jnp.sum(states[None, :] < docs[:, None], axis=1, dtype=jnp.int32)
    state_last = jnp.sum(states[None, :] <= docs[:, None], axis=1, dtype=jnp.int32) - 1
    own_base = (2 * chip + core) * rows
    other_base = (2 * chip + 1 - core) * rows
    at = jnp.concatenate(
        [
            own_base + jnp.arange(rows, dtype=jnp.int32),
            other_base + jnp.arange(rows, dtype=jnp.int32),
        ]
    )
    ids_here = jnp.concatenate(
        [
            lax.dynamic_slice_in_dim(ids, own_base, rows),
            lax.dynamic_slice_in_dim(ids, other_base, rows),
        ]
    )
    lo = pick(ids_here, starts)
    cross_lo = pick(ids_here, state_first)
    cross_hi = pick(ids_here, state_last)
    first, last = slice(0, None, Q_TILE), slice(Q_TILE - 1, None, Q_TILE)
    blocks = jnp.arange(4 * rows // self_tile, dtype=jnp.int32)
    place = blocks * self_tile
    part = place // rows
    held = jnp.where(part // 2 == chip, 2, 0) + ((part % 2) ^ core)
    self_off = held * rows + place % rows
    self_table = jnp.concatenate([lo[first] // self_tile, at[last] // self_tile + 1, self_off])
    cross_off = jnp.arange(states.shape[0] // cross_tile, dtype=jnp.int32) * cross_tile
    cross_table = jnp.concatenate(
        [cross_lo[first] // cross_tile, cross_hi[last] // cross_tile + 1, cross_off]
    )
    return (
        (self_table, lo[None], at[None]),
        (cross_table, cross_lo[None], cross_hi[None]),
    )


SELF_TILE = 256
CROSS_TILE = 128


def body(
    widened_in,
    encoder_states,
    predict,
    correct_gain,
    self_gain,
    self_q,
    self_k,
    self_v,
    self_o,
    cross_gain,
    cross_q,
    cross_k,
    cross_v,
    cross_o,
    ffn_gain,
    ffn_gate,
    ffn_up,
    ffn_down,
    segment_ids,
    encoder_ids,
    block_choice,
    out_grad,
):
    rows = widened_in.shape[0]
    half_width = widened_in.shape[1] // 2
    head_cols = self_q.shape[1]
    hidden_cols = ffn_gate.shape[1]

    def fetch(w_query, w_key, w_value, w_out):
        first = gather_weight(jnp.concatenate([w_query, w_key], axis=1), True)
        second = gather_weight(jnp.concatenate([w_value, w_out], axis=1), False)
        return (
            [s[:, :head_cols] for s in first],
            [s[:, head_cols:] for s in first],
            [s[:, :head_cols] for s in second],
            [s[:, head_cols:] for s in second],
        )

    half_hidden = hidden_cols // 2
    sq, sk, sv, so = fetch(self_q, self_k, self_v, self_o)
    cq, ck, cv, co = fetch(cross_q, cross_k, cross_v, cross_o)
    wg = gather_weight(ffn_gate, True)
    wu = gather_weight(ffn_up, False)
    down_first = gather_weight(ffn_down[:, :half_hidden], True)
    down_second = gather_weight(ffn_down[:, half_hidden:], False)
    wd = [jnp.concatenate([a, b], axis=1) for a, b in zip(down_first, down_second)]

    (self_table, self_lo, self_hi), (cross_table, cross_lo, cross_hi) = key_tables(
        segment_ids, encoder_ids, rows, SELF_TILE, CROSS_TILE
    )

    widened = widened_in.astype(f32)
    first_block = widened[:, :half_width]
    second_block = widened[:, half_width:]
    picked = (block_choice == 1)[:, None]
    pred_first = predict[0, 0] * first_block + predict[0, 1] * second_block
    pred_second = predict[1, 0] * first_block + predict[1, 1] * second_block
    pred_chosen = jnp.where(picked, pred_second, pred_first)
    chosen = jnp.where(picked, second_block, first_block)
    d_out = out_grad.astype(f32)
    d_first = d_out[:, :half_width]
    d_second = d_out[:, half_width:]
    d_computed = correct_gain[0] * d_first + correct_gain[1] * d_second

    normed_own = rms_forward(chosen, self_gain).astype(bf16)
    before = lax.ppermute(normed_own, "ty", [(0, 1)])
    normed_self = pair_rows(normed_own)
    source = jnp.concatenate([pair_rows(before), normed_self], axis=0)
    d_branch_ffn = pair_rows(d_computed.astype(bf16))

    core = lax.axis_index("core")
    swapped = swap_core(encoder_states)
    states = jnp.concatenate(
        [
            jnp.where(core == 0, encoder_states, swapped),
            jnp.where(core == 0, swapped, encoder_states),
        ],
        axis=0,
    )
    far = swap_ty(states)
    chip = lax.axis_index("ty")
    encoder = jnp.concatenate(
        [jnp.where(chip == 0, states, far), jnp.where(chip == 0, far, states)], axis=0
    )

    self_queries = [mdot(normed_self, w).astype(bf16) for w in sq]
    self_keys = [mdot(source, w).astype(bf16) for w in sk]
    self_values = [mdot(source, w).astype(bf16) for w in sv]
    self_mix0, self_mix1, self_lse = attention_forward(
        self_table, self_lo, self_hi, self_queries, self_keys, self_values, SELF_TILE
    )
    self_mix = [self_mix0, self_mix1]

    def branch_out(mixes, outs):
        return lambda lo, hi: ndot(mixes[0][lo:hi], outs[0]) + ndot(mixes[1][lo:hi], outs[1])

    after_self = chosen + pair_sum(branch_out(self_mix, so), rows)

    cross_keys = [mdot(encoder, w).astype(bf16) for w in ck]
    cross_values = [mdot(encoder, w).astype(bf16) for w in cv]
    normed_cross = pair_rows(rms_forward(after_self, cross_gain).astype(bf16))
    cross_queries = [mdot(normed_cross, w).astype(bf16) for w in cq]
    cross_mix0, cross_mix1, cross_lse = attention_forward(
        cross_table, cross_lo, cross_hi, cross_queries, cross_keys, cross_values, CROSS_TILE
    )
    cross_mix = [cross_mix0, cross_mix1]
    after_cross = after_self + pair_sum(branch_out(cross_mix, co), rows)

    normed_ffn = pair_rows(rms_forward(after_cross, ffn_gain).astype(bf16))
    gates = [mdot(normed_ffn, w) for w in wg]
    ups = [mdot(normed_ffn, w) for w in wu]

    def gelu_mix(gate, up_rows):
        return jax.nn.gelu(gate, approximate=True) * up_rows

    hidden = [gelu_mix(g, u).astype(bf16) for g, u in zip(gates, ups)]
    computed = after_cross + pair_sum(branch_out(hidden, wd), rows)

    gap = computed - pred_chosen
    widened_out = jnp.concatenate(
        [pred_first + correct_gain[0] * gap, pred_second + correct_gain[1] * gap], axis=1
    ).astype(bf16)
    gain_terms = jnp.stack([jnp.sum(d_first * gap), jnp.sum(d_second * gap)])
    d_pred_first = d_first - jnp.where(picked, 0.0, d_computed)
    d_pred_second = d_second - jnp.where(picked, d_computed, 0.0)

    d_gates, d_ups = [], []
    for slab in range(2):
        d_hidden = mdot(d_branch_ffn, wd[slab])
        unused, pullback = jax.vjp(gelu_mix, gates[slab], ups[slab])
        d_gate, d_up = pullback(d_hidden)
        d_gates.append(d_gate.astype(bf16))
        d_ups.append(d_up.astype(bf16))

    def ffn_back(lo, hi):
        return (
            ndot(d_gates[0][lo:hi], wg[0])
            + ndot(d_ups[0][lo:hi], wu[0])
            + ndot(d_gates[1][lo:hi], wg[1])
            + ndot(d_ups[1][lo:hi], wu[1])
        )

    d_normed_ffn = pair_sum(ffn_back, rows)
    down_parts = [tdot(d_branch_ffn, h).astype(bf16) for h in hidden]
    gate_parts = [tdot(normed_ffn, d).astype(bf16) for d in d_gates]
    up_parts = [tdot(normed_ffn, d).astype(bf16) for d in d_ups]
    ffn_gate_grad = reduce_weight(gate_parts, True)
    ffn_up_grad = reduce_weight(up_parts, False)
    ffn_down_grad = jnp.concatenate(
        [
            reduce_weight([p[:, :half_hidden] for p in down_parts], True),
            reduce_weight([p[:, half_hidden:] for p in down_parts], False),
        ],
        axis=1,
    )
    d_cross_rows, ffn_gain_part = rms_backward(after_cross, ffn_gain, d_normed_ffn)
    d_after_cross = d_computed + d_cross_rows

    d_branch = pair_rows(d_after_cross.astype(bf16))
    d_mix = [mdot(d_branch, w).astype(bf16) for w in co]
    cross_o_parts = [tdot(d_branch, m).astype(bf16) for m in cross_mix]
    d_query, d_keys, d_values = attention_backward(
        cross_table,
        cross_lo,
        cross_hi,
        cross_lse,
        cross_queries,
        d_mix,
        cross_mix,
        cross_keys,
        cross_values,
        CROSS_TILE,
    )
    d_normed_cross = pair_sum(branch_out(d_query, cq), rows)
    d_encoder = (
        ndot(d_keys[0], ck[0])
        + ndot(d_keys[1], ck[1])
        + ndot(d_values[0], cv[0])
        + ndot(d_values[1], cv[1])
    ).astype(bf16)
    quarter = d_encoder.reshape((2, 2) + encoder_states.shape)
    kept = lax.dynamic_index_in_dim(quarter, chip, 0, keepdims=False)
    sent = lax.dynamic_index_in_dim(quarter, 1 - chip, 0, keepdims=False)
    kept = plus(kept, swap_ty(sent))
    mine = lax.dynamic_index_in_dim(kept, core, 0, keepdims=False)
    theirs = lax.dynamic_index_in_dim(kept, 1 - core, 0, keepdims=False)
    encoder_grad = mine.astype(f32) + swap_core(theirs).astype(f32)

    def reduce_attention(q_parts, k_parts, v_parts, o_parts):
        first = reduce_weight(
            [jnp.concatenate([a, b], axis=1) for a, b in zip(q_parts, k_parts)], True
        )
        second = reduce_weight(
            [jnp.concatenate([a, b], axis=1) for a, b in zip(v_parts, o_parts)], False
        )
        return (
            first[:, :head_cols],
            first[:, head_cols:],
            second[:, :head_cols],
            second[:, head_cols:],
        )

    cross_q_grad, cross_k_grad, cross_v_grad, cross_o_grad = reduce_attention(
        [tdot(normed_cross, d).astype(bf16) for d in d_query],
        [tdot(encoder, d).astype(bf16) for d in d_keys],
        [tdot(encoder, d).astype(bf16) for d in d_values],
        cross_o_parts,
    )
    d_self_rows, cross_gain_part = rms_backward(after_self, cross_gain, d_normed_cross)
    d_after_self = d_after_cross + d_self_rows

    d_branch = pair_rows(d_after_self.astype(bf16))
    d_mix = [mdot(d_branch, w).astype(bf16) for w in so]
    self_o_parts = [tdot(d_branch, m).astype(bf16) for m in self_mix]
    d_query, d_keys, d_values = attention_backward(
        self_table,
        self_lo,
        self_hi,
        self_lse,
        self_queries,
        d_mix,
        self_mix,
        self_keys,
        self_values,
        SELF_TILE,
    )

    def source_back(lo, hi):
        return (
            ndot(d_keys[0][lo:hi], sk[0])
            + ndot(d_keys[1][lo:hi], sk[1])
            + ndot(d_values[0][lo:hi], sv[0])
            + ndot(d_values[1][lo:hi], sv[1])
        )

    d_before = pair_sum(source_back, rows).astype(bf16)
    d_later = lax.ppermute(d_before, "ty", [(1, 0)])

    def own_back(lo, hi):
        return branch_out(d_query, sq)(lo, hi) + source_back(2 * rows + lo, 2 * rows + hi)

    d_normed_self = pair_sum(own_back, rows) + d_later.astype(f32)
    self_q_grad, self_k_grad, self_v_grad, self_o_grad = reduce_attention(
        [tdot(normed_self, d).astype(bf16) for d in d_query],
        [tdot(source, d).astype(bf16) for d in d_keys],
        [tdot(source, d).astype(bf16) for d in d_values],
        self_o_parts,
    )
    d_chosen_rows, self_gain_part = rms_backward(chosen, self_gain, d_normed_self)
    d_chosen = d_after_self + d_chosen_rows
    first_grad = (
        predict[0, 0] * d_pred_first
        + predict[1, 0] * d_pred_second
        + jnp.where(picked, 0.0, d_chosen)
    )
    second_grad = (
        predict[0, 1] * d_pred_first
        + predict[1, 1] * d_pred_second
        + jnp.where(picked, d_chosen, 0.0)
    )
    input_grad = jnp.concatenate([first_grad, second_grad], axis=1)
    terms = jnp.stack(
        [
            jnp.sum(d_pred_first * first_block),
            jnp.sum(d_pred_first * second_block),
            jnp.sum(d_pred_second * first_block),
            jnp.sum(d_pred_second * second_block),
            gain_terms[0],
            gain_terms[1],
        ]
    )
    packed = jnp.zeros((4, half_width), f32)
    packed = packed.at[0].set(self_gain_part).at[1].set(cross_gain_part)
    packed = packed.at[2].set(ffn_gain_part).at[3, :6].set(terms)
    packed = sum_everywhere(packed)
    return (
        widened_out,
        input_grad,
        encoder_grad,
        packed[3, :4].reshape(2, 2),
        packed[3, 4:6],
        packed[0],
        self_q_grad,
        self_k_grad,
        self_v_grad,
        self_o_grad,
        packed[1],
        cross_q_grad,
        cross_k_grad,
        cross_v_grad,
        cross_o_grad,
        packed[2],
        ffn_gate_grad,
        ffn_up_grad,
        ffn_down_grad,
    )


def solution(mesh):
    dp, tensor = mesh.shape["dp"], mesh.shape["tensor"]
    split = Mesh(mesh.devices.reshape(dp, tensor // 2, 2), ("dp", "ty", "core"))
    tokens = P(("dp", "ty", "core"), None)
    weight = P("dp", ("ty", "core"))
    full = P()
    in_specs = (
        (tokens, tokens, full, full)
        + (full, weight, weight, weight, weight) * 2
        + (full, weight, weight, weight)
        + (P("dp", None), P("dp", None), P(("dp", "ty", "core")), tokens)
    )
    out_specs = (
        (tokens, tokens, tokens, full, full)
        + (full, weight, weight, weight, weight) * 2
        + (full, weight, weight, weight)
    )
    return jax.shard_map(body, mesh=split, in_specs=in_specs, out_specs=out_specs, check_vma=False)
```

```python
import functools
import jax
import jax.numpy as jnp
from jax import lax
from jax.experimental import pallas as pl
from jax.experimental.pallas import tpu as pltpu
from jax.sharding import Mesh, PartitionSpec as P

HDIM = 64
DOCS = 6
epsilon = 1e-06
f32 = jnp.float32
bf16 = jnp.bfloat16
NEG = -1e30
Q_TILE = 256


def tdot(left_mat, right_mat):
    return lax.dot_general(
        left_mat, right_mat, (((0,), (0,)), ((), ())), preferred_element_type=f32
    )


def ndot(left_mat, right_mat):
    return lax.dot_general(
        left_mat, right_mat, (((1,), (1,)), ((), ())), preferred_element_type=f32
    )


def mdot(left_mat, right_mat):
    return jnp.dot(left_mat, right_mat, preferred_element_type=f32)


def rms_forward(values, norm_gain):
    factor = lax.rsqrt(jnp.mean(values * values, axis=-1, keepdims=True) + epsilon)
    return values * factor * norm_gain


def rms_backward(values, norm_gain, d_normed):
    factor = lax.rsqrt(jnp.mean(values * values, axis=-1, keepdims=True) + epsilon)
    scaled = d_normed * norm_gain
    d_values = factor * scaled - values * factor * factor * factor * jnp.mean(
        scaled * values, axis=-1, keepdims=True
    )
    gain_grad = jnp.sum(d_normed * values * factor, axis=0)
    return (d_values, gain_grad)


def swap_core(rows):
    return lax.ppermute(rows, "core", [(0, 1), (1, 0)])


def swap_ty(rows):
    return lax.ppermute(rows, "ty", [(0, 1), (1, 0)])


def swap_bit(rows, bit):
    size = lax.axis_size("dp")
    return lax.ppermute(rows, "dp", [(i, i ^ (1 << bit)) for i in range(size)])


def my_bit(bit):
    return (lax.axis_index("dp") >> bit) & 1


def dp_bits():
    return lax.axis_size("dp").bit_length() - 1


def plus(left_mat, right_mat):
    return (left_mat.astype(f32) + right_mat.astype(f32)).astype(bf16)


def shrink(partial, bit, left):
    at = sum(1 for known in left if known > bit)
    mine = my_bit(bit)
    sent = lax.dynamic_index_in_dim(partial, 1 - mine, at, keepdims=False)
    kept = lax.dynamic_index_in_dim(partial, mine, at, keepdims=False)
    return plus(kept, swap_bit(sent, bit))


def reduce_weight(slabs, y_first):
    bits = dp_bits()
    size = lax.axis_size("dp")
    rows, cols = slabs[0].shape
    shaped = [s.reshape((2,) * bits + (rows // size, cols)) for s in slabs]
    left = list(range(bits))
    if y_first:
        total = plus(shaped[0], swap_ty(shaped[1]))
        total = shrink(total, 0, left)
    else:
        shaped = [shrink(s, 0, left) for s in shaped]
        total = plus(shaped[0], swap_ty(shaped[1]))
    left.remove(0)
    for bit in reversed(range(1, bits)):
        total = shrink(total, bit, left)
        left.remove(bit)
    return total.astype(f32)


def sum_everywhere(values):
    for bit in range(dp_bits()):
        values = values + swap_bit(values, bit)
    values = values + swap_ty(values)
    return values + swap_core(values)


def pair_rows(own_rows):
    return jnp.concatenate([own_rows, swap_core(own_rows)], axis=0)


def pair_sum(part, rows):
    sent = part(rows, 2 * rows).astype(bf16)
    arrived = swap_core(sent)
    return part(0, rows) + arrived.astype(f32)


def gather_kernel(bits, packs, *refs):
    pieces, outs = refs[:packs], refs[packs : 2 * packs]
    local_sem, send_sem, recv_sem = refs[2 * packs :]
    me = lax.axis_index("dp")
    chip = lax.axis_index("ty")
    own = [(me >> bit) & 1 for bit in range(bits)]
    partners = [{"dp": me ^ (1 << bit)} for bit in range(bits)] + [{"ty": 1 - chip}]
    barrier = pltpu.get_barrier_semaphore()
    for partner in partners:
        pl.semaphore_signal(
            barrier, inc=1, device_id=partner, device_id_type=pl.DeviceIdType.MESH
        )
    locals_ = []
    for pack in range(packs):
        at = (0,) + tuple(own[bit] for bit in reversed(range(bits)))
        copy = pltpu.make_async_copy(pieces[pack], outs[pack].at[at], local_sem.at[pack])
        copy.start()
        locals_.append(copy)
    for copy in locals_:
        copy.wait()
    pl.semaphore_wait(barrier, bits + 1)

    inner = list(range(1, bits))
    orders = (inner + [0, bits], inner + [bits, 0])
    cols = pieces[0].shape[1] // 2
    stages = bits + 1
    everything = []
    flights = {}

    def region(order, gen, sent_to_y):
        where = []
        for dim in [bits] + list(reversed(range(bits))):
            at = order.index(dim)
            if at < gen - 1:
                where.append(slice(None))
            elif dim == bits:
                where.append(1 if at == gen - 1 or sent_to_y else 0)
            else:
                where.append(1 - own[dim] if at == gen - 1 else own[dim])
        return tuple(where)

    for gen in range(stages + 1):
        for pack in range(packs):
            for color, order in enumerate(orders):
                lanes = (slice(None), slice(color * cols, (color + 1) * cols))
                if gen > 0:
                    for copy in flights[pack, color, gen - 1]:
                        copy.wait_recv()
                for stage in range(gen, stages):
                    dim = order[stage]
                    source = outs[pack].at[region(order, gen, False) + lanes]
                    target = outs[pack].at[region(order, gen, dim == bits) + lanes]
                    slot = ((pack * 2 + color) * stages + stage) * stages + gen
                    copy = pltpu.make_async_remote_copy(
                        src_ref=source,
                        dst_ref=target,
                        send_sem=send_sem.at[slot],
                        recv_sem=recv_sem.at[slot],
                        device_id=partners[dim],
                        device_id_type=pl.DeviceIdType.MESH,
                    )
                    copy.start()
                    everything.append(copy)
                    flights.setdefault((pack, color, stage), []).append(copy)
    for copy in everything:
        copy.wait_send()


def gather_attention(packed):
    bits = dp_bits()
    rows, cols = packed[0].shape
    packs = len(packed)
    slots = packs * 2 * (bits + 1) * (bits + 1)
    shape = jax.ShapeDtypeStruct((2,) * (bits + 1) + (rows, cols), bf16)
    out = pl.pallas_call(
        functools.partial(gather_kernel, bits, packs),
        out_shape=(shape,) * packs,
        in_specs=[pl.BlockSpec(memory_space=pltpu.VMEM)] * packs,
        out_specs=(pl.BlockSpec(memory_space=pl.ANY),) * packs,
        scratch_shapes=[
            pltpu.SemaphoreType.DMA((packs,)),
            pltpu.SemaphoreType.DMA((slots,)),
            pltpu.SemaphoreType.DMA((slots,)),
        ],
        compiler_params=pltpu.CompilerParams(collective_id=0, has_side_effects=True),
        name="gather_attention",
    )(*packed)
    return [o.reshape(2, -1, cols) for o in out]


KEY_LANES = ((128, 256), (256, 384), (256, 384))
VALUE_LANES = ((384, 512), (384, 512), (512, 576))


def lane_half(block, high):
    lane = lax.broadcasted_iota(jnp.int32, block.shape, 1)
    return jnp.where((lane >= HDIM) == high, block, jnp.zeros_like(block))


def query_parts(block):
    scaled = block.astype(f32) * 0.125
    turned = pltpu.roll(scaled[:, 0:128], HDIM, 1).astype(bf16)
    third = pltpu.roll(scaled[:, 128:256], HDIM, 1).astype(bf16)
    return [lane_half(turned, True), lane_half(turned, False), lane_half(third, True)]


QUERY_ROWS = (slice(HDIM, None), slice(0, HDIM), slice(HDIM, None))


def grad_parts(block):
    pair = block[:, 0:128]
    return [lane_half(pair, False), lane_half(pair, True), block[:, 128:192]]


VALUE_ROWS = (slice(0, HDIM), slice(HDIM, None), slice(0, HDIM))


def allowed_keys(key_base, tile, lo, hi):
    key_at = lax.broadcasted_iota(jnp.int32, (tile, lo.shape[1]), 0) + key_base
    return jnp.logical_and(key_at >= lo, key_at <= hi)


def key_range(lo, hi, tile):
    first = jnp.min(lo.astype(f32)).astype(jnp.int32)
    last = jnp.max(hi.astype(f32)).astype(jnp.int32)
    return first // tile, last // tile + 1


def key_offset(at, tile, rows, causal):
    if not causal:
        return pl.multiple_of(at * tile, tile)
    place = at * tile
    part = place // rows
    held = jnp.where(part // 2 == lax.axis_index("ty"), 2, 0)
    held = held + jnp.where(part % 2 == lax.axis_index("core"), 0, 1)
    return pl.multiple_of(held * rows + place % rows, tile)


def forward_kernel(tile, rows, causal, q0, q1, p0, p1, info, mix0, mix1, lse_ref, acc, peak, total):
    base = 0 if causal else 2
    lo, hi = info[base : base + 1, :], info[base + 1 : base + 2, :]
    acc[...] = jnp.zeros_like(acc)
    peak[...] = jnp.full_like(peak, NEG)
    total[...] = jnp.zeros_like(total)
    queries = [query_parts(q[...]) for q in (q0, q1)]
    first_tile, end_tile = key_range(lo, hi, tile)

    def one(at, carry):
        off = key_offset(at, tile, rows, causal)
        allow = allowed_keys(at * tile, tile, lo, hi)
        for slab, ref in enumerate((p0, p1)):
            for head in range(3):
                row = slab * 3 + head
                keys = ref[pl.ds(off, tile), slice(*KEY_LANES[head])]
                values = ref[pl.ds(off, tile), slice(*VALUE_LANES[head])]
                scores = jnp.where(allow, ndot(keys, queries[slab][head]), NEG)
                old = peak[row : row + 1, :]
                top = jnp.maximum(old, jnp.max(scores, axis=0, keepdims=True))
                weights = jnp.exp(scores - top)
                fade = jnp.exp(old - top)
                total[row : row + 1, :] = total[row : row + 1, :] * fade + jnp.sum(
                    weights, axis=0, keepdims=True
                )
                peak[row : row + 1, :] = top
                fresh = tdot(values, weights.astype(bf16))[VALUE_ROWS[head], :]
                span = slice(row * HDIM, (row + 1) * HDIM)
                acc[span, :] = acc[span, :] * fade + fresh
        return carry

    lax.fori_loop(first_tile, end_tile, one, 0)
    lse_ref[...] = peak[...] + jnp.log(total[...])
    for slab, mix in enumerate((mix0, mix1)):
        pieces = []
        for head in range(3):
            row = slab * 3 + head
            pieces.append(acc[row * HDIM : (row + 1) * HDIM, :] / total[row : row + 1, :])
        mix[...] = jnp.concatenate(pieces, axis=0).T.astype(bf16)


def backward_kernel(tile, rows, causal, q0, q1, g0, g1, mix0, mix1, p0, p1, info, lse_ref, *refs):
    if causal:
        dp0, dp1, acc, wide0, wide1 = refs
    else:
        dq0, dq1, dp0, dp1, acc, wide0, wide1 = refs
    step = pl.program_id(0)
    base = 0 if causal else 2
    lo, hi = info[base : base + 1, :], info[base + 1 : base + 2, :]

    @pl.when(step == 0)
    def _():
        wide0[...] = jnp.zeros_like(wide0)
        wide1[...] = jnp.zeros_like(wide1)

    acc[...] = jnp.zeros_like(acc)
    queries = [query_parts(q[...]) for q in (q0, q1)]
    grads = [grad_parts(g[...]) for g in (g0, g1)]
    inner = []
    for g, mix in ((g0, mix0), (g1, mix1)):
        both = (g[...].astype(f32) * mix[...].astype(f32)).T
        for head in range(3):
            inner.append(
                jnp.sum(both[head * HDIM : (head + 1) * HDIM, :], axis=0, keepdims=True)
            )
    first_tile, end_tile = key_range(lo, hi, tile)

    def one(at, carry):
        off = key_offset(at, tile, rows, causal)
        allow = allowed_keys(at * tile, tile, lo, hi)
        for slab, (ref, wide) in enumerate(((p0, wide0), (p1, wide1))):
            for head in range(3):
                row = slab * 3 + head
                key_at = (pl.ds(off, tile), slice(*KEY_LANES[head]))
                value_at = (pl.ds(off, tile), slice(*VALUE_LANES[head]))
                keys, values = ref[key_at], ref[value_at]
                query, grad = queries[slab][head], grads[slab][head]
                scores = ndot(keys, query) - lse_ref[row : row + 1, :]
                probs = jnp.exp(jnp.where(allow, scores, NEG))
                d_probs = ndot(values, grad)
                d_scores = (probs * (d_probs - inner[row])).astype(bf16)
                wide[value_at] += mdot(probs.astype(bf16), grad)
                wide[key_at] += mdot(d_scores, query)
                span = slice(row * HDIM, (row + 1) * HDIM)
                acc[span, :] += tdot(keys, d_scores)[QUERY_ROWS[head], :]
        return carry

    lax.fori_loop(first_tile, end_tile, one, 0)
    count = acc.shape[1]
    for slab in range(2):
        d_query = (acc[slab * 192 : (slab + 1) * 192, :] * 0.125).T
        if causal:
            at = pl.ds(pl.multiple_of(2 * rows + step * count, count), count)
            (wide0, wide1)[slab][at, 0:192] = d_query
        else:
            (dq0, dq1)[slab][:, 0:192] = d_query.astype(bf16)
            (dq0, dq1)[slab][:, 192:256] = jnp.zeros((count, HDIM), bf16)

    @pl.when(step == pl.num_programs(0) - 1)
    def _():
        dp0[...] = wide0[...].astype(bf16)
        dp1[...] = wide1[...].astype(bf16)


def attention_specs(packed, rows, causal):
    total, cols = packed[0].shape
    skip = 2 * rows // Q_TILE if causal else 0
    query_block = pl.BlockSpec((Q_TILE, 256), lambda i: (i + skip, 0))
    row_block = pl.BlockSpec((Q_TILE, 192), lambda i: (i, 0))
    packed_block = pl.BlockSpec((total, cols), lambda i: (0, 0))
    lane_block = pl.BlockSpec((8, Q_TILE), lambda i: (0, i))
    return total, cols, query_block, row_block, packed_block, lane_block


def attention_forward(queries, packed, info, rows, tile, causal):
    total, cols, query_block, row_block, packed_block, lane_block = attention_specs(
        packed, rows, causal
    )
    work = 2 * rows * total * 384
    return pl.pallas_call(
        functools.partial(forward_kernel, tile, rows, causal),
        out_shape=(
            jax.ShapeDtypeStruct((2 * rows, 192), bf16),
            jax.ShapeDtypeStruct((2 * rows, 192), bf16),
            jax.ShapeDtypeStruct((8, 2 * rows), f32),
        ),
        grid=(2 * rows // Q_TILE,),
        in_specs=[query_block] * 2 + [packed_block] * 2 + [lane_block],
        out_specs=(row_block, row_block, lane_block),
        scratch_shapes=[
            pltpu.VMEM((384, Q_TILE), f32),
            pltpu.VMEM((8, Q_TILE), f32),
            pltpu.VMEM((8, Q_TILE), f32),
        ],
        compiler_params=pltpu.CompilerParams(
            dimension_semantics=("arbitrary",), vmem_limit_bytes=32 << 20
        ),
        cost_estimate=pl.CostEstimate(
            flops=4 * work, bytes_accessed=4 * total * cols, transcendentals=work // 64
        ),
        name="attend_forward",
    )(*queries, *packed, info)


def attention_backward(queries, grads, mixes, packed, info, lse, rows, tile, causal):
    total, cols, query_block, row_block, packed_block, lane_block = attention_specs(
        packed, rows, causal
    )
    work = 2 * rows * total * 384
    out_shape = [jax.ShapeDtypeStruct((total, cols), bf16)] * 2
    out_specs = [packed_block] * 2
    if not causal:
        out_shape = [jax.ShapeDtypeStruct((2 * rows, 256), bf16)] * 2 + out_shape
        out_specs = [query_block] * 2 + out_specs
    out = pl.pallas_call(
        functools.partial(backward_kernel, tile, rows, causal),
        out_shape=tuple(out_shape),
        grid=(2 * rows // Q_TILE,),
        in_specs=[query_block] * 2 + [row_block] * 4 + [packed_block] * 2 + [lane_block] * 2,
        out_specs=tuple(out_specs),
        scratch_shapes=[pltpu.VMEM((384, Q_TILE), f32)] + [pltpu.VMEM((total, cols), f32)] * 2,
        compiler_params=pltpu.CompilerParams(
            dimension_semantics=("arbitrary",), vmem_limit_bytes=56 << 20
        ),
        cost_estimate=pl.CostEstimate(
            flops=10 * work, bytes_accessed=8 * total * cols, transcendentals=work // 64
        ),
        name="attend_backward",
    )(*queries, *grads, *mixes, *packed, info, lse)
    return (None, out) if causal else (out[:2], out[2:])


def table_kernel(rows, ids_ref, states_ref, info):
    chip, core = lax.axis_index("ty"), lax.axis_index("core")
    ids, states = ids_ref[...], states_ref[...]
    info[...] = jnp.zeros_like(info)

    def count(flags):
        return jnp.sum(flags.astype(f32), axis=1, keepdims=True).astype(jnp.int32)

    for half in range(2):
        base = (2 * chip + jnp.where(core == half, 0, 1)) * rows
        here = ids_ref[:, pl.ds(pl.multiple_of(base, rows), rows)]
        lo = jnp.zeros_like(here)
        cross_lo, cross_hi = lo, lo
        for doc in range(DOCS):
            same = here == doc
            lo = jnp.where(same, count(ids < doc), lo)
            cross_lo = jnp.where(same, count(states < doc), cross_lo)
            cross_hi = jnp.where(same, count(states <= doc) - 1, cross_hi)
        span = slice(half * rows, (half + 1) * rows)
        info[0:1, span] = lo
        info[1:2, span] = base + lax.broadcasted_iota(jnp.int32, here.shape, 1)
        info[2:3, span] = cross_lo
        info[3:4, span] = cross_hi


def key_tables(segment_ids, encoder_ids, rows):
    return pl.pallas_call(
        functools.partial(table_kernel, rows),
        out_shape=jax.ShapeDtypeStruct((8, 2 * rows), jnp.int32),
        in_specs=[pl.BlockSpec(memory_space=pltpu.VMEM)] * 2,
        out_specs=pl.BlockSpec(memory_space=pltpu.VMEM),
        name="key_tables",
    )(segment_ids, encoder_ids)


SELF_TILE = 256
CROSS_TILE = 128


def body(
    widened_in,
    encoder_states,
    predict,
    correct_gain,
    self_gain,
    self_q,
    self_k,
    self_v,
    self_o,
    cross_gain,
    cross_q,
    cross_k,
    cross_v,
    cross_o,
    ffn_gain,
    ffn_gate,
    ffn_up,
    ffn_down,
    segment_ids,
    encoder_ids,
    block_choice,
    out_grad,
):
    rows = widened_in.shape[0]
    half_width = widened_in.shape[1] // 2
    head_cols = self_q.shape[1]
    hidden_cols = ffn_gate.shape[1]

    self_w, cross_w = gather_attention(
        [
            jnp.concatenate([self_q, self_k, self_v, self_o], axis=1),
            jnp.concatenate([cross_q, cross_k, cross_v, cross_o], axis=1),
        ]
    )
    ffn_w = lax.all_gather(
        jnp.concatenate([ffn_gate, ffn_up, ffn_down], axis=1), ("ty", "dp"), axis=0, tiled=True
    ).reshape(2, -1, 3 * hidden_cols)
    wg = [ffn_w[j, :, :hidden_cols] for j in range(2)]
    wu = [ffn_w[j, :, hidden_cols : 2 * hidden_cols] for j in range(2)]
    wd = [ffn_w[j, :, 2 * hidden_cols :] for j in range(2)]
    sw = [self_w[j] for j in range(2)]
    cw = [cross_w[j] for j in range(2)]
    so = [w[:, 3 * head_cols :] for w in sw]
    co = [w[:, 3 * head_cols :] for w in cw]
    cq = [w[:, :256] for w in cw]
    info = key_tables(segment_ids, encoder_ids, rows)

    widened = widened_in.astype(f32)
    first_block = widened[:, :half_width]
    second_block = widened[:, half_width:]
    picked = (block_choice == 1)[:, None]
    pred_first = predict[0, 0] * first_block + predict[0, 1] * second_block
    pred_second = predict[1, 0] * first_block + predict[1, 1] * second_block
    pred_chosen = jnp.where(picked, pred_second, pred_first)
    chosen = jnp.where(picked, second_block, first_block)
    d_out = out_grad.astype(f32)
    d_first = d_out[:, :half_width]
    d_second = d_out[:, half_width:]
    d_computed = correct_gain[0] * d_first + correct_gain[1] * d_second

    normed_own = rms_forward(chosen, self_gain).astype(bf16)
    before = lax.ppermute(normed_own, "ty", [(0, 1)])
    normed_self = pair_rows(normed_own)
    source = jnp.concatenate([pair_rows(before), normed_self], axis=0)
    d_branch_ffn = pair_rows(d_computed.astype(bf16))

    core = lax.axis_index("core")
    swapped = swap_core(encoder_states)
    states = jnp.concatenate(
        [
            jnp.where(core == 0, encoder_states, swapped),
            jnp.where(core == 0, swapped, encoder_states),
        ],
        axis=0,
    )
    far = swap_ty(states)
    chip = lax.axis_index("ty")
    encoder = jnp.concatenate(
        [jnp.where(chip == 0, states, far), jnp.where(chip == 0, far, states)], axis=0
    )

    self_packed = [mdot(source, w).astype(bf16) for w in sw]
    self_mix0, self_mix1, self_lse = attention_forward(
        self_packed, self_packed, info, rows, SELF_TILE, True
    )
    self_mix = [self_mix0, self_mix1]

    def branch_out(mixes, outs):
        return lambda lo, hi: ndot(mixes[0][lo:hi], outs[0]) + ndot(mixes[1][lo:hi], outs[1])

    after_self = chosen + pair_sum(branch_out(self_mix, so), rows)

    cross_packed = [mdot(encoder, w).astype(bf16) for w in cw]
    normed_cross = pair_rows(rms_forward(after_self, cross_gain).astype(bf16))
    cross_queries = [mdot(normed_cross, w).astype(bf16) for w in cq]
    cross_mix0, cross_mix1, cross_lse = attention_forward(
        cross_queries, cross_packed, info, rows, CROSS_TILE, False
    )
    cross_mix = [cross_mix0, cross_mix1]
    after_cross = after_self + pair_sum(branch_out(cross_mix, co), rows)

    normed_ffn = pair_rows(rms_forward(after_cross, ffn_gain).astype(bf16))
    gates = [mdot(normed_ffn, w) for w in wg]
    ups = [mdot(normed_ffn, w) for w in wu]

    def gelu_mix(gate, up_rows):
        return jax.nn.gelu(gate, approximate=True) * up_rows

    hidden = [gelu_mix(g, u).astype(bf16) for g, u in zip(gates, ups)]
    computed = after_cross + pair_sum(branch_out(hidden, wd), rows)

    gap = computed - pred_chosen
    widened_out = jnp.concatenate(
        [pred_first + correct_gain[0] * gap, pred_second + correct_gain[1] * gap], axis=1
    ).astype(bf16)
    gain_terms = jnp.stack([jnp.sum(d_first * gap), jnp.sum(d_second * gap)])
    d_pred_first = d_first - jnp.where(picked, 0.0, d_computed)
    d_pred_second = d_second - jnp.where(picked, d_computed, 0.0)

    d_gates, d_ups = [], []
    for slab in range(2):
        d_hidden = mdot(d_branch_ffn, wd[slab])
        unused, pullback = jax.vjp(gelu_mix, gates[slab], ups[slab])
        d_gate, d_up = pullback(d_hidden)
        d_gates.append(d_gate.astype(bf16))
        d_ups.append(d_up.astype(bf16))

    def ffn_back(lo, hi):
        return (
            ndot(d_gates[0][lo:hi], wg[0])
            + ndot(d_ups[0][lo:hi], wu[0])
            + ndot(d_gates[1][lo:hi], wg[1])
            + ndot(d_ups[1][lo:hi], wu[1])
        )

    d_normed_ffn = pair_sum(ffn_back, rows)
    ffn_parts = jnp.concatenate(
        [
            jnp.concatenate(
                [
                    tdot(normed_ffn, d_gates[j]).astype(bf16),
                    tdot(normed_ffn, d_ups[j]).astype(bf16),
                    tdot(d_branch_ffn, hidden[j]).astype(bf16),
                ],
                axis=1,
            )
            for j in range(2)
        ],
        axis=0,
    )
    ffn_grads = lax.psum_scatter(
        ffn_parts, ("ty", "dp"), scatter_dimension=0, tiled=True
    ).astype(f32)
    d_cross_rows, ffn_gain_part = rms_backward(after_cross, ffn_gain, d_normed_ffn)
    d_after_cross = d_computed + d_cross_rows

    d_branch = pair_rows(d_after_cross.astype(bf16))
    d_mix = [mdot(d_branch, w).astype(bf16) for w in co]
    cross_o_parts = [tdot(d_branch, m).astype(bf16) for m in cross_mix]
    d_query, d_packed = attention_backward(
        cross_queries, d_mix, cross_mix, cross_packed, info, cross_lse, rows, CROSS_TILE, False
    )
    d_normed_cross = pair_sum(branch_out(d_query, cq), rows)
    d_encoder = (ndot(d_packed[0], cw[0]) + ndot(d_packed[1], cw[1])).astype(bf16)
    quarter = d_encoder.reshape((2, 2) + encoder_states.shape)
    kept = lax.dynamic_index_in_dim(quarter, chip, 0, keepdims=False)
    sent = lax.dynamic_index_in_dim(quarter, 1 - chip, 0, keepdims=False)
    kept = plus(kept, swap_ty(sent))
    mine = lax.dynamic_index_in_dim(kept, core, 0, keepdims=False)
    theirs = lax.dynamic_index_in_dim(kept, 1 - core, 0, keepdims=False)
    encoder_grad = mine.astype(f32) + swap_core(theirs).astype(f32)

    def reduce_attention(parts):
        half = 2 * head_cols
        first = reduce_weight([p[:, :half] for p in parts], True)
        second = reduce_weight([p[:, half:] for p in parts], False)
        return (
            first[:, :head_cols],
            first[:, head_cols:],
            second[:, :head_cols],
            second[:, head_cols:],
        )

    cross_parts = []
    for slab in range(2):
        query_part = tdot(normed_cross, d_query[slab]).astype(bf16)
        state_part = tdot(encoder, d_packed[slab]).astype(bf16)
        cross_parts.append(
            jnp.concatenate(
                [
                    query_part[:, :head_cols],
                    state_part[:, head_cols : 3 * head_cols],
                    cross_o_parts[slab],
                ],
                axis=1,
            )
        )
    cross_q_grad, cross_k_grad, cross_v_grad, cross_o_grad = reduce_attention(cross_parts)
    d_self_rows, cross_gain_part = rms_backward(after_self, cross_gain, d_normed_cross)
    d_after_self = d_after_cross + d_self_rows

    d_branch = pair_rows(d_after_self.astype(bf16))
    d_mix = [mdot(d_branch, w).astype(bf16) for w in so]
    self_o_parts = [tdot(d_branch, m).astype(bf16) for m in self_mix]
    unused, d_packed = attention_backward(
        self_packed, d_mix, self_mix, self_packed, info, self_lse, rows, SELF_TILE, True
    )
    source_back = branch_out(d_packed, sw)
    d_before = pair_sum(source_back, rows).astype(bf16)
    d_later = lax.ppermute(d_before, "ty", [(1, 0)])

    def own_back(lo, hi):
        return source_back(2 * rows + lo, 2 * rows + hi)

    d_normed_self = pair_sum(own_back, rows) + d_later.astype(f32)
    self_parts = [
        jnp.concatenate(
            [tdot(source, d_packed[j]).astype(bf16)[:, : 3 * head_cols], self_o_parts[j]], axis=1
        )
        for j in range(2)
    ]
    self_q_grad, self_k_grad, self_v_grad, self_o_grad = reduce_attention(self_parts)
    d_chosen_rows, self_gain_part = rms_backward(chosen, self_gain, d_normed_self)
    d_chosen = d_after_self + d_chosen_rows
    first_grad = (
        predict[0, 0] * d_pred_first
        + predict[1, 0] * d_pred_second
        + jnp.where(picked, 0.0, d_chosen)
    )
    second_grad = (
        predict[0, 1] * d_pred_first
        + predict[1, 1] * d_pred_second
        + jnp.where(picked, d_chosen, 0.0)
    )
    input_grad = jnp.concatenate([first_grad, second_grad], axis=1)
    terms = jnp.stack(
        [
            jnp.sum(d_pred_first * first_block),
            jnp.sum(d_pred_first * second_block),
            jnp.sum(d_pred_second * first_block),
            jnp.sum(d_pred_second * second_block),
            gain_terms[0],
            gain_terms[1],
        ]
    )
    packed = jnp.zeros((4, half_width), f32)
    packed = packed.at[0].set(self_gain_part).at[1].set(cross_gain_part)
    packed = packed.at[2].set(ffn_gain_part).at[3, :6].set(terms)
    packed = sum_everywhere(packed)
    return (
        widened_out,
        input_grad,
        encoder_grad,
        packed[3, :4].reshape(2, 2),
        packed[3, 4:6],
        packed[0],
        self_q_grad,
        self_k_grad,
        self_v_grad,
        self_o_grad,
        packed[1],
        cross_q_grad,
        cross_k_grad,
        cross_v_grad,
        cross_o_grad,
        packed[2],
        ffn_grads[:, :hidden_cols],
        ffn_grads[:, hidden_cols : 2 * hidden_cols],
        ffn_grads[:, 2 * hidden_cols :],
    )


def solution(mesh):
    dp, tensor = mesh.shape["dp"], mesh.shape["tensor"]
    split = Mesh(mesh.devices.reshape(dp, tensor // 2, 2), ("dp", "ty", "core"))
    tokens = P(("dp", "ty", "core"), None)
    weight = P("dp", ("ty", "core"))
    full = P()
    in_specs = (
        (tokens, tokens, full, full)
        + (full, weight, weight, weight, weight) * 2
        + (full, weight, weight, weight)
        + (P("dp", None), P("dp", None), P(("dp", "ty", "core")), tokens)
    )
    out_specs = (
        (tokens, tokens, tokens, full, full)
        + (full, weight, weight, weight, weight) * 2
        + (full, weight, weight, weight)
    )
    return jax.shard_map(body, mesh=split, in_specs=in_specs, out_specs=out_specs, check_vma=False)
```

```python
import functools
import jax
import jax.numpy as jnp
from jax import lax
from jax.experimental import pallas as pl
from jax.experimental.pallas import tpu as pltpu
from jax.sharding import Mesh, PartitionSpec as P

HDIM = 64
DOCS = 6
epsilon = 1e-06
f32 = jnp.float32
bf16 = jnp.bfloat16
NEG = -1e30
Q_TILE = 256


def tdot(left_mat, right_mat):
    return lax.dot_general(
        left_mat, right_mat, (((0,), (0,)), ((), ())), preferred_element_type=f32
    )


def ndot(left_mat, right_mat):
    return lax.dot_general(
        left_mat, right_mat, (((1,), (1,)), ((), ())), preferred_element_type=f32
    )


def mdot(left_mat, right_mat):
    return jnp.dot(left_mat, right_mat, preferred_element_type=f32)


def rms_forward(values, norm_gain):
    factor = lax.rsqrt(jnp.mean(values * values, axis=-1, keepdims=True) + epsilon)
    return values * factor * norm_gain


def rms_backward(values, norm_gain, d_normed):
    factor = lax.rsqrt(jnp.mean(values * values, axis=-1, keepdims=True) + epsilon)
    scaled = d_normed * norm_gain
    d_values = factor * scaled - values * factor * factor * factor * jnp.mean(
        scaled * values, axis=-1, keepdims=True
    )
    gain_grad = jnp.sum(d_normed * values * factor, axis=0)
    return (d_values, gain_grad)


def swap_core(rows):
    return lax.ppermute(rows, "core", [(0, 1), (1, 0)])


def swap_ty(rows):
    return lax.ppermute(rows, "ty", [(0, 1), (1, 0)])


def swap_bit(rows, bit):
    size = lax.axis_size("dp")
    return lax.ppermute(rows, "dp", [(i, i ^ (1 << bit)) for i in range(size)])


def my_bit(bit):
    return (lax.axis_index("dp") >> bit) & 1


def dp_bits():
    return lax.axis_size("dp").bit_length() - 1


def plus(left_mat, right_mat):
    return (left_mat.astype(f32) + right_mat.astype(f32)).astype(bf16)


def pair_rows(own_rows):
    return jnp.concatenate([own_rows, swap_core(own_rows)], axis=0)


def pair_sum(part, rows):
    sent = part(rows, 2 * rows).astype(bf16)
    arrived = swap_core(sent)
    return part(0, rows) + arrived.astype(f32)


def gather_kernel(bits, packs, *refs):
    pieces, outs = refs[:packs], refs[packs : 2 * packs]
    local_sem, send_sem, recv_sem = refs[2 * packs :]
    me = lax.axis_index("dp")
    chip = lax.axis_index("ty")
    own = [(me >> bit) & 1 for bit in range(bits)]
    partners = [{"dp": me ^ (1 << bit)} for bit in range(bits)] + [{"ty": 1 - chip}]
    barrier = pltpu.get_barrier_semaphore()
    for partner in partners:
        pl.semaphore_signal(
            barrier, inc=1, device_id=partner, device_id_type=pl.DeviceIdType.MESH
        )
    locals_ = []
    for pack in range(packs):
        at = (0,) + tuple(own[bit] for bit in reversed(range(bits)))
        copy = pltpu.make_async_copy(pieces[pack], outs[pack].at[at], local_sem.at[pack])
        copy.start()
        locals_.append(copy)
    for copy in locals_:
        copy.wait()
    pl.semaphore_wait(barrier, bits + 1)

    inner = list(range(1, bits))
    orders = (inner + [0, bits], inner + [bits, 0])
    cols = pieces[0].shape[1] // 2
    stages = bits + 1
    everything = []
    flights = {}

    def region(order, gen, sent_to_y):
        where = []
        for dim in [bits] + list(reversed(range(bits))):
            at = order.index(dim)
            if at < gen - 1:
                where.append(slice(None))
            elif dim == bits:
                where.append(1 if at == gen - 1 or sent_to_y else 0)
            else:
                where.append(1 - own[dim] if at == gen - 1 else own[dim])
        return tuple(where)

    for gen in range(stages + 1):
        for pack in range(packs):
            for color, order in enumerate(orders):
                lanes = (slice(None), slice(color * cols, (color + 1) * cols))
                if gen > 0:
                    for copy in flights[pack, color, gen - 1]:
                        copy.wait_recv()
                for stage in range(gen, stages):
                    dim = order[stage]
                    source = outs[pack].at[region(order, gen, False) + lanes]
                    target = outs[pack].at[region(order, gen, dim == bits) + lanes]
                    slot = ((pack * 2 + color) * stages + stage) * stages + gen
                    copy = pltpu.make_async_remote_copy(
                        src_ref=source,
                        dst_ref=target,
                        send_sem=send_sem.at[slot],
                        recv_sem=recv_sem.at[slot],
                        device_id=partners[dim],
                        device_id_type=pl.DeviceIdType.MESH,
                    )
                    copy.start()
                    everything.append(copy)
                    flights.setdefault((pack, color, stage), []).append(copy)
    for copy in everything:
        copy.wait_send()


def gather_attention(packed):
    bits = dp_bits()
    rows, cols = packed[0].shape
    packs = len(packed)
    slots = packs * 2 * (bits + 1) * (bits + 1)
    shape = jax.ShapeDtypeStruct((2,) * (bits + 1) + (rows, cols), bf16)
    out = pl.pallas_call(
        functools.partial(gather_kernel, bits, packs),
        out_shape=(shape,) * packs,
        in_specs=[pl.BlockSpec(memory_space=pltpu.VMEM)] * packs,
        out_specs=(pl.BlockSpec(memory_space=pl.ANY),) * packs,
        scratch_shapes=[
            pltpu.SemaphoreType.DMA((packs,)),
            pltpu.SemaphoreType.DMA((slots,)),
            pltpu.SemaphoreType.DMA((slots,)),
        ],
        compiler_params=pltpu.CompilerParams(collective_id=0, has_side_effects=True),
        cost_estimate=pl.CostEstimate(flops=0, bytes_accessed=150 << 20, transcendentals=0),
        name="gather_attention",
    )(*packed)
    return [o.reshape(2, -1, cols) for o in out]


def reduce_kernel(bits, packs, *refs):
    parts, small, outs = refs[:packs], refs[packs], refs[packs + 1 : 2 * packs + 1]
    small_out = refs[2 * packs + 1]
    works = refs[2 * packs + 2 : 3 * packs + 2]
    lands = refs[3 * packs + 2 : 4 * packs + 2]
    vectors, vector_lands, send_sem, recv_sem, vector_send, vector_recv = refs[4 * packs + 2 :]
    me, chip, core = lax.axis_index("dp"), lax.axis_index("ty"), lax.axis_index("core")
    own = [(me >> bit) & 1 for bit in range(bits)]
    partners = [{"dp": me ^ (1 << bit)} for bit in range(bits)] + [
        {"ty": 1 - chip},
        {"core": 1 - core},
    ]
    barrier = pltpu.get_barrier_semaphore()
    for partner in partners:
        pl.semaphore_signal(
            barrier, inc=1, device_id=partner, device_id_type=pl.DeviceIdType.MESH
        )
    vectors[0] = small[...]
    pl.semaphore_wait(barrier, bits + 2)

    inner = list(reversed(range(1, bits)))
    orders = ([bits, 0] + inner, [0, bits] + inner)
    cols = parts[0].shape[-1] // 2
    stages = bits + 1
    everything, flights = [], {}

    def spot(choice, flip):
        where = []
        for dim in [bits] + list(reversed(range(bits))):
            side = choice.get(dim)
            if side is None:
                where.append(slice(None))
            elif dim == bits:
                where.append(side)
            else:
                at = own[dim] if side == 0 else 1 - own[dim]
                where.append(1 - at if dim == flip else at)
        return tuple(where)

    def message(order, stage, sub):
        choice = {order[i]: 0 for i in range(stage)}
        choice[order[stage]] = 1
        for i in range(stage + 1, sub):
            choice[order[i]] = 0
        if sub < stages:
            choice[order[sub]] = 1
        return choice

    def lanes_of(color):
        return (slice(None), slice(color * cols, (color + 1) * cols))

    def send(pack, color, stage):
        order = orders[color]
        source = parts[pack] if stage == 0 else works[pack]
        for sub in range(stage + 1, stages + 1):
            choice = message(order, stage, sub)
            slot = ((pack * 2 + color) * stages + stage) * stages + sub - 1
            copy = pltpu.make_async_remote_copy(
                src_ref=source.at[spot(choice, None) + lanes_of(color)],
                dst_ref=lands[pack].at[spot(choice, order[stage]) + lanes_of(color)],
                send_sem=send_sem.at[slot],
                recv_sem=recv_sem.at[slot],
                device_id=partners[order[stage]],
                device_id_type=pl.DeviceIdType.MESH,
            )
            copy.start()
            everything.append(copy)
            flights[pack, color, stage, sub] = copy

    def collect(pack, color, sub):
        order = orders[color]
        choice = {order[i]: 0 for i in range(sub)}
        if sub < stages:
            choice[order[sub]] = 1
        here = spot(choice, None) + lanes_of(color)
        total = parts[pack][here].astype(f32)
        for stage in range(sub):
            flights[pack, color, stage, sub].wait_recv()
            there = spot(message(order, stage, sub), None) + lanes_of(color)
            total = total + lands[pack][there].astype(f32)
        return here, total

    def vector_start(step):
        copy = pltpu.make_async_remote_copy(
            src_ref=vectors.at[step],
            dst_ref=vector_lands.at[step],
            send_sem=vector_send.at[step],
            recv_sem=vector_recv.at[step],
            device_id=partners[step],
            device_id_type=pl.DeviceIdType.MESH,
        )
        copy.start()
        everything.append(copy)
        return copy

    pairs = [(pack, color) for pack in range(packs) for color in range(2)]
    for pack, color in pairs:
        send(pack, color, 0)
    vector = vector_start(0)
    step = 0
    for sub in range(1, stages + 1):
        for pack, color in pairs:
            here, total = collect(pack, color, sub)
            if sub < stages:
                works[pack][here] = total.astype(bf16)
                send(pack, color, sub)
            else:
                outs[pack][lanes_of(color)] = total
            if step < bits + 2:
                vector.wait_recv()
                vectors[step + 1] = vectors[step] + vector_lands[step]
                step += 1
                if step < bits + 2:
                    vector = vector_start(step)
    small_out[...] = vectors[bits + 2]
    for copy in everything:
        copy.wait_send()


def reduce_attention(parts, small):
    bits = dp_bits()
    packs = len(parts)
    size = lax.axis_size("dp")
    whole, cols = parts[0].shape[1:]
    blocks = (2,) * (bits + 1) + (whole // size, cols)
    slots = packs * 2 * (bits + 1) * (bits + 1)
    vmem = pl.BlockSpec(memory_space=pltpu.VMEM)
    out = pl.pallas_call(
        functools.partial(reduce_kernel, bits, packs),
        out_shape=(jax.ShapeDtypeStruct((whole // size, cols), f32),) * packs
        + (jax.ShapeDtypeStruct(small.shape, f32),),
        in_specs=[vmem] * (packs + 1),
        out_specs=(vmem,) * (packs + 1),
        scratch_shapes=[pltpu.VMEM(blocks, bf16)] * (2 * packs)
        + [
            pltpu.VMEM((bits + 3,) + small.shape, f32),
            pltpu.VMEM((bits + 2,) + small.shape, f32),
            pltpu.SemaphoreType.DMA((slots,)),
            pltpu.SemaphoreType.DMA((slots,)),
            pltpu.SemaphoreType.DMA((bits + 2,)),
            pltpu.SemaphoreType.DMA((bits + 2,)),
        ],
        compiler_params=pltpu.CompilerParams(
            collective_id=1, has_side_effects=True, vmem_limit_bytes=56 << 20
        ),
        cost_estimate=pl.CostEstimate(flops=0, bytes_accessed=150 << 20, transcendentals=0),
        name="reduce_attention",
    )(*[p.reshape(blocks) for p in parts], small)
    return out[:packs], out[packs]


ROW_CHUNK = 512


def attention_grad_kernel(spans, *refs):
    count = len(spans)
    lefts, rights, out, acc = refs[:count], refs[count : 3 * count], refs[3 * count], refs[-1]
    for slab in range(2):

        @pl.when(pl.program_id(0) == slab)
        def _():
            for term, (first, last) in enumerate(spans):
                left, right = lefts[term], rights[2 * term + slab]
                for at in range(0, left.shape[0], ROW_CHUNK):
                    chunk = slice(at, at + ROW_CHUNK)
                    product = tdot(left[chunk, :], right[chunk, :])
                    if term == 0 and at == 0:
                        acc[...] = product
                    else:
                        acc[:, first:last] += product

    out[0] = acc[...].astype(bf16)


def attention_grad(terms):
    spans = tuple(span for left, rights, span in terms)
    lefts = [left for left, rights, span in terms]
    rights = [r for left, pair, span in terms for r in pair]
    whole, cols = lefts[0].shape[1], rights[0].shape[1]
    flops = 4 * whole * sum(t[0].shape[0] * t[1][0].shape[1] for t in terms)
    return pl.pallas_call(
        functools.partial(attention_grad_kernel, spans),
        out_shape=jax.ShapeDtypeStruct((2, whole, cols), bf16),
        grid=(2,),
        in_specs=[pl.BlockSpec(x.shape, lambda i: (0, 0)) for x in lefts + rights],
        out_specs=pl.BlockSpec((1, whole, cols), lambda i: (i, 0, 0)),
        scratch_shapes=[pltpu.VMEM((whole, cols), f32)],
        compiler_params=pltpu.CompilerParams(
            dimension_semantics=("arbitrary",), vmem_limit_bytes=56 << 20
        ),
        cost_estimate=pl.CostEstimate(
            flops=flops, bytes_accessed=16 * whole * cols, transcendentals=0
        ),
        name="attention_grad",
    )(*lefts, *rights)


def ffn_grad_kernel(kinds, *refs):
    lefts, rights, out = refs[:kinds], refs[kinds : 3 * kinds], refs[-1]
    for slab in range(2):
        for kind in range(kinds):

            @pl.when(
                jnp.logical_and(pl.program_id(0) == slab, pl.program_id(1) == kind)
            )
            def _():
                left, right = lefts[kind], rights[slab * kinds + kind]
                out[...] = tdot(left[...], right[...]).astype(bf16)


def ffn_grad(lefts, rights):
    kinds = len(lefts)
    rows, whole = lefts[0].shape
    cols = rights[0].shape[1]
    return pl.pallas_call(
        functools.partial(ffn_grad_kernel, kinds),
        out_shape=jax.ShapeDtypeStruct((2 * whole, kinds * cols), bf16),
        grid=(2, kinds),
        in_specs=[pl.BlockSpec(x.shape, lambda i, k: (0, 0)) for x in list(lefts) + list(rights)],
        out_specs=pl.BlockSpec((whole, cols), lambda i, k: (i, k)),
        compiler_params=pltpu.CompilerParams(
            dimension_semantics=("arbitrary", "arbitrary"), vmem_limit_bytes=56 << 20
        ),
        cost_estimate=pl.CostEstimate(
            flops=4 * kinds * rows * whole * cols,
            bytes_accessed=2 * kinds * (2 * rows + 2 * whole) * cols,
            transcendentals=0,
        ),
        name="ffn_grad",
    )(*lefts, *rights)


KEY_LANES = ((128, 256), (256, 384), (256, 384))
VALUE_LANES = ((384, 512), (384, 512), (512, 640))


def lane_half(block, high):
    lane = lax.broadcasted_iota(jnp.int32, block.shape, 1)
    return jnp.where((lane >= HDIM) == high, block, jnp.zeros_like(block))


def query_parts(block):
    scaled = block.astype(f32) * 0.125
    turned = pltpu.roll(scaled[:, 0:128], HDIM, 1).astype(bf16)
    third = pltpu.roll(scaled[:, 128:256], HDIM, 1).astype(bf16)
    return [lane_half(turned, True), lane_half(turned, False), lane_half(third, True)]


QUERY_ROWS = (slice(HDIM, None), slice(0, HDIM), slice(HDIM, None))


def grad_parts(block):
    wide = block.astype(f32)
    turned = pltpu.roll(wide[:, 0:128], HDIM, 1).astype(bf16)
    others = pltpu.roll(wide[:, 128:256], HDIM, 1).astype(bf16)
    return [lane_half(turned, False), lane_half(others, True), lane_half(others, False)]


VALUE_ROWS = (slice(0, HDIM), slice(HDIM, None), slice(0, HDIM))


def allowed_keys(key_base, tile, lo, hi):
    key_at = lax.broadcasted_iota(jnp.int32, (tile, lo.shape[1]), 0) + key_base
    return jnp.logical_and(key_at >= lo, key_at <= hi)


def key_range(lo, hi, tile):
    first = jnp.min(lo.astype(f32)).astype(jnp.int32)
    last = jnp.max(hi.astype(f32)).astype(jnp.int32)
    return first // tile, last // tile + 1


def key_offset(at, tile, rows, causal):
    if not causal:
        return pl.multiple_of(at * tile, tile)
    place = at * tile
    part = place // rows
    held = jnp.where(part // 2 == lax.axis_index("ty"), 2, 0)
    held = held + jnp.where(part % 2 == lax.axis_index("core"), 0, 1)
    return pl.multiple_of(held * rows + place % rows, tile)


def forward_kernel(tile, rows, causal, q0, q1, p0, p1, info, mix0, mix1, lse_ref, acc):
    base = 0 if causal else 2
    lo, hi = info[base : base + 1, :], info[base + 1 : base + 2, :]
    acc[...] = jnp.zeros_like(acc)
    queries = [part for q in (q0, q1) for part in query_parts(q[...])]
    first_tile, end_tile = key_range(lo, hi, tile)
    heads = range(6)

    def one(at, carry):
        peaks, totals = carry
        off = key_offset(at, tile, rows, causal)
        allow = allowed_keys(at * tile, tile, lo, hi)
        scores, values = [], []
        for row in heads:
            ref = (p0, p1)[row // 3]
            keys = ref[pl.ds(off, tile), slice(*KEY_LANES[row % 3])]
            values.append(ref[pl.ds(off, tile), slice(*VALUE_LANES[row % 3])])
            scores.append(jnp.where(allow, ndot(keys, queries[row]), NEG))
        tops = [
            jnp.maximum(peaks[row], jnp.max(scores[row], axis=0, keepdims=True)) for row in heads
        ]
        fades = [jnp.exp(peaks[row] - tops[row]) for row in heads]
        fresh_totals = []
        for row in heads:
            weights = jnp.exp(scores[row] - tops[row])
            fresh_totals.append(
                totals[row] * fades[row] + jnp.sum(weights, axis=0, keepdims=True)
            )
            fresh = tdot(values[row], weights.astype(bf16))[VALUE_ROWS[row % 3], :]
            span = slice(row * HDIM, (row + 1) * HDIM)
            acc[span, :] = acc[span, :] * fades[row] + fresh
        return (tuple(tops), tuple(fresh_totals))

    start = (
        tuple(jnp.full(lo.shape, NEG, f32) for row in heads),
        tuple(jnp.zeros(lo.shape, f32) for row in heads),
    )
    peaks, totals = lax.fori_loop(first_tile, end_tile, one, start)
    lse_ref[...] = jnp.zeros_like(lse_ref)
    for row in heads:
        lse_ref[row : row + 1, :] = peaks[row] + jnp.log(totals[row])
    for slab, mix in enumerate((mix0, mix1)):
        pieces = [jnp.zeros((HDIM, acc.shape[1]), f32)]
        for row in range(slab * 3, slab * 3 + 3):
            pieces.append(acc[row * HDIM : (row + 1) * HDIM, :] / totals[row])
        mix[...] = jnp.concatenate(pieces, axis=0).T.astype(bf16)


def backward_kernel(tile, rows, causal, q0, q1, g0, g1, mix0, mix1, p0, p1, info, lse_ref, *refs):
    if causal:
        dp0, dp1, acc, wide0, wide1 = refs
    else:
        dq0, dq1, dp0, dp1, acc, wide0, wide1 = refs
    step = pl.program_id(0)
    base = 0 if causal else 2
    lo, hi = info[base : base + 1, :], info[base + 1 : base + 2, :]

    @pl.when(step == 0)
    def _():
        wide0[...] = jnp.zeros_like(wide0)
        wide1[...] = jnp.zeros_like(wide1)

    acc[...] = jnp.zeros_like(acc)
    queries = [query_parts(q[...]) for q in (q0, q1)]
    grads = [grad_parts(g[...]) for g in (g0, g1)]
    inner = []
    for g, mix in ((g0, mix0), (g1, mix1)):
        both = (g[...].astype(f32) * mix[...].astype(f32)).T
        for head in range(3):
            inner.append(
                jnp.sum(both[(head + 1) * HDIM : (head + 2) * HDIM, :], axis=0, keepdims=True)
            )
    first_tile, end_tile = key_range(lo, hi, tile)

    def one(at, carry):
        off = key_offset(at, tile, rows, causal)
        allow = allowed_keys(at * tile, tile, lo, hi)
        for slab, (ref, wide) in enumerate(((p0, wide0), (p1, wide1))):
            for head in range(3):
                row = slab * 3 + head
                key_at = (pl.ds(off, tile), slice(*KEY_LANES[head]))
                value_at = (pl.ds(off, tile), slice(*VALUE_LANES[head]))
                keys, values = ref[key_at], ref[value_at]
                query, grad = queries[slab][head], grads[slab][head]
                scores = ndot(keys, query) - lse_ref[row : row + 1, :]
                probs = jnp.exp(jnp.where(allow, scores, NEG))
                d_probs = ndot(values, grad)
                d_scores = (probs * (d_probs - inner[row])).astype(bf16)
                wide[value_at] += mdot(probs.astype(bf16), grad)
                wide[key_at] += mdot(d_scores, query)
                span = slice(row * HDIM, (row + 1) * HDIM)
                acc[span, :] += tdot(keys, d_scores)[QUERY_ROWS[head], :]
        return carry

    lax.fori_loop(first_tile, end_tile, one, 0)
    count = acc.shape[1]
    for slab in range(2):
        d_query = (acc[slab * 192 : (slab + 1) * 192, :] * 0.125).T
        if causal:
            at = pl.ds(pl.multiple_of(2 * rows + step * count, count), count)
            (wide0, wide1)[slab][at, 0:192] = d_query
        else:
            (dq0, dq1)[slab][:, 0:192] = d_query.astype(bf16)
            (dq0, dq1)[slab][:, 192:256] = jnp.zeros((count, HDIM), bf16)

    @pl.when(step == pl.num_programs(0) - 1)
    def _():
        dp0[...] = wide0[...].astype(bf16)
        dp1[...] = wide1[...].astype(bf16)


def attention_specs(packed, rows, causal):
    total, cols = packed[0].shape
    skip = 2 * rows // Q_TILE if causal else 0
    query_block = pl.BlockSpec((Q_TILE, 256), lambda i: (i + skip, 0))
    row_block = pl.BlockSpec((Q_TILE, 256), lambda i: (i, 0))
    packed_block = pl.BlockSpec((total, cols), lambda i: (0, 0))
    lane_block = pl.BlockSpec((8, Q_TILE), lambda i: (0, i))
    return total, cols, query_block, row_block, packed_block, lane_block


def attention_forward(queries, packed, info, rows, tile, causal):
    total, cols, query_block, row_block, packed_block, lane_block = attention_specs(
        packed, rows, causal
    )
    work = 2 * rows * total * 384
    return pl.pallas_call(
        functools.partial(forward_kernel, tile, rows, causal),
        out_shape=(
            jax.ShapeDtypeStruct((2 * rows, 256), bf16),
            jax.ShapeDtypeStruct((2 * rows, 256), bf16),
            jax.ShapeDtypeStruct((8, 2 * rows), f32),
        ),
        grid=(2 * rows // Q_TILE,),
        in_specs=[query_block] * 2 + [packed_block] * 2 + [lane_block],
        out_specs=(row_block, row_block, lane_block),
        scratch_shapes=[pltpu.VMEM((384, Q_TILE), f32)],
        compiler_params=pltpu.CompilerParams(
            dimension_semantics=("arbitrary",), vmem_limit_bytes=32 << 20
        ),
        cost_estimate=pl.CostEstimate(
            flops=4 * work, bytes_accessed=4 * total * cols, transcendentals=work // 64
        ),
        name="attend_forward",
    )(*queries, *packed, info)


def attention_backward(queries, grads, mixes, packed, info, lse, rows, tile, causal):
    total, cols, query_block, row_block, packed_block, lane_block = attention_specs(
        packed, rows, causal
    )
    work = 2 * rows * total * 384
    out_shape = [jax.ShapeDtypeStruct((total, cols), bf16)] * 2
    out_specs = [packed_block] * 2
    if not causal:
        out_shape = [jax.ShapeDtypeStruct((2 * rows, 256), bf16)] * 2 + out_shape
        out_specs = [query_block] * 2 + out_specs
    out = pl.pallas_call(
        functools.partial(backward_kernel, tile, rows, causal),
        out_shape=tuple(out_shape),
        grid=(2 * rows // Q_TILE,),
        in_specs=[query_block] * 2 + [row_block] * 4 + [packed_block] * 2 + [lane_block] * 2,
        out_specs=tuple(out_specs),
        scratch_shapes=[pltpu.VMEM((384, Q_TILE), f32)] + [pltpu.VMEM((total, cols), f32)] * 2,
        compiler_params=pltpu.CompilerParams(
            dimension_semantics=("arbitrary",), vmem_limit_bytes=56 << 20
        ),
        cost_estimate=pl.CostEstimate(
            flops=10 * work, bytes_accessed=8 * total * cols, transcendentals=work // 64
        ),
        name="attend_backward",
    )(*queries, *grads, *mixes, *packed, info, lse)
    return (None, out) if causal else (out[:2], out[2:])


def table_kernel(rows, ids_ref, states_ref, info):
    chip, core = lax.axis_index("ty"), lax.axis_index("core")
    ids, states = ids_ref[...], states_ref[...]
    info[...] = jnp.zeros_like(info)

    def count(flags):
        return jnp.sum(flags.astype(f32), axis=1, keepdims=True).astype(jnp.int32)

    for half in range(2):
        base = (2 * chip + jnp.where(core == half, 0, 1)) * rows
        here = ids_ref[:, pl.ds(pl.multiple_of(base, rows), rows)]
        lo = jnp.zeros_like(here)
        cross_lo, cross_hi = lo, lo
        for doc in range(DOCS):
            same = here == doc
            lo = jnp.where(same, count(ids < doc), lo)
            cross_lo = jnp.where(same, count(states < doc), cross_lo)
            cross_hi = jnp.where(same, count(states <= doc) - 1, cross_hi)
        span = slice(half * rows, (half + 1) * rows)
        info[0:1, span] = lo
        info[1:2, span] = base + lax.broadcasted_iota(jnp.int32, here.shape, 1)
        info[2:3, span] = cross_lo
        info[3:4, span] = cross_hi


def key_tables(segment_ids, encoder_ids, rows):
    return pl.pallas_call(
        functools.partial(table_kernel, rows),
        out_shape=jax.ShapeDtypeStruct((8, 2 * rows), jnp.int32),
        in_specs=[pl.BlockSpec(memory_space=pltpu.VMEM)] * 2,
        out_specs=pl.BlockSpec(memory_space=pltpu.VMEM),
        name="key_tables",
    )(segment_ids, encoder_ids)


SELF_TILE = 256
CROSS_TILE = 128


def body(
    widened_in,
    encoder_states,
    predict,
    correct_gain,
    self_gain,
    self_q,
    self_k,
    self_v,
    self_o,
    cross_gain,
    cross_q,
    cross_k,
    cross_v,
    cross_o,
    ffn_gain,
    ffn_gate,
    ffn_up,
    ffn_down,
    segment_ids,
    encoder_ids,
    block_choice,
    out_grad,
):
    rows = widened_in.shape[0]
    half_width = widened_in.shape[1] // 2
    head_cols = self_q.shape[1]
    hidden_cols = ffn_gate.shape[1]

    self_w, cross_w = gather_attention(
        [
            jnp.concatenate([self_q, self_k, self_v, self_o], axis=1),
            jnp.concatenate([cross_q, cross_k, cross_v, cross_o], axis=1),
        ]
    )
    ffn_w = lax.all_gather(
        jnp.concatenate([ffn_gate, ffn_up, ffn_down], axis=1), ("ty", "dp"), axis=0, tiled=True
    ).reshape(2, -1, 3 * hidden_cols)
    wg = [ffn_w[j, :, :hidden_cols] for j in range(2)]
    wu = [ffn_w[j, :, hidden_cols : 2 * hidden_cols] for j in range(2)]
    wd = [ffn_w[j, :, 2 * hidden_cols :] for j in range(2)]
    sw = [self_w[j] for j in range(2)]
    cw = [cross_w[j] for j in range(2)]
    so = [w[:, 512:] for w in sw]
    co = [w[:, 512:] for w in cw]
    cq = [w[:, :256] for w in cw]
    info = key_tables(segment_ids, encoder_ids, rows)

    widened = widened_in.astype(f32)
    first_block = widened[:, :half_width]
    second_block = widened[:, half_width:]
    picked = (block_choice == 1)[:, None]
    pred_first = predict[0, 0] * first_block + predict[0, 1] * second_block
    pred_second = predict[1, 0] * first_block + predict[1, 1] * second_block
    pred_chosen = jnp.where(picked, pred_second, pred_first)
    chosen = jnp.where(picked, second_block, first_block)
    d_out = out_grad.astype(f32)
    d_first = d_out[:, :half_width]
    d_second = d_out[:, half_width:]
    d_computed = correct_gain[0] * d_first + correct_gain[1] * d_second

    normed_own = rms_forward(chosen, self_gain).astype(bf16)
    before = lax.ppermute(normed_own, "ty", [(0, 1)])
    normed_self = pair_rows(normed_own)
    source = jnp.concatenate([pair_rows(before), normed_self], axis=0)
    d_branch_ffn = pair_rows(d_computed.astype(bf16))

    core = lax.axis_index("core")
    swapped = swap_core(encoder_states)
    states = jnp.concatenate(
        [
            jnp.where(core == 0, encoder_states, swapped),
            jnp.where(core == 0, swapped, encoder_states),
        ],
        axis=0,
    )
    far = swap_ty(states)
    chip = lax.axis_index("ty")
    encoder = jnp.concatenate(
        [jnp.where(chip == 0, states, far), jnp.where(chip == 0, far, states)], axis=0
    )

    self_packed = [mdot(source, w).astype(bf16) for w in sw]
    self_mix0, self_mix1, self_lse = attention_forward(
        self_packed, self_packed, info, rows, SELF_TILE, True
    )
    self_mix = [self_mix0, self_mix1]

    def branch_out(mixes, outs):
        return lambda lo, hi: ndot(mixes[0][lo:hi], outs[0]) + ndot(mixes[1][lo:hi], outs[1])

    after_self = chosen + pair_sum(branch_out(self_mix, so), rows)

    cross_packed = [mdot(encoder, w).astype(bf16) for w in cw]
    normed_cross = pair_rows(rms_forward(after_self, cross_gain).astype(bf16))
    cross_queries = [mdot(normed_cross, w).astype(bf16) for w in cq]
    cross_mix0, cross_mix1, cross_lse = attention_forward(
        cross_queries, cross_packed, info, rows, CROSS_TILE, False
    )
    cross_mix = [cross_mix0, cross_mix1]
    after_cross = after_self + pair_sum(branch_out(cross_mix, co), rows)

    normed_ffn = pair_rows(rms_forward(after_cross, ffn_gain).astype(bf16))
    gates = [mdot(normed_ffn, w) for w in wg]
    ups = [mdot(normed_ffn, w) for w in wu]

    def gelu_mix(gate, up_rows):
        return jax.nn.gelu(gate, approximate=True) * up_rows

    hidden = [gelu_mix(g, u).astype(bf16) for g, u in zip(gates, ups)]
    computed = after_cross + pair_sum(branch_out(hidden, wd), rows)

    gap = computed - pred_chosen
    widened_out = jnp.concatenate(
        [pred_first + correct_gain[0] * gap, pred_second + correct_gain[1] * gap], axis=1
    ).astype(bf16)
    d_pred_first = d_first - jnp.where(picked, 0.0, d_computed)
    d_pred_second = d_second - jnp.where(picked, d_computed, 0.0)

    d_gates, d_ups = [], []
    for slab in range(2):
        d_hidden = mdot(d_branch_ffn, wd[slab])
        unused, pullback = jax.vjp(gelu_mix, gates[slab], ups[slab])
        d_gate, d_up = pullback(d_hidden)
        d_gates.append(d_gate.astype(bf16))
        d_ups.append(d_up.astype(bf16))

    def ffn_back(lo, hi):
        return (
            ndot(d_gates[0][lo:hi], wg[0])
            + ndot(d_ups[0][lo:hi], wu[0])
            + ndot(d_gates[1][lo:hi], wg[1])
            + ndot(d_ups[1][lo:hi], wu[1])
        )

    d_normed_ffn = pair_sum(ffn_back, rows)
    ffn_parts = ffn_grad(
        [normed_ffn, normed_ffn, d_branch_ffn],
        [d_gates[0], d_ups[0], hidden[0], d_gates[1], d_ups[1], hidden[1]],
    )
    ffn_grads = lax.psum_scatter(
        ffn_parts, ("ty", "dp"), scatter_dimension=0, tiled=True
    ).astype(f32)
    d_cross_rows, ffn_gain_part = rms_backward(after_cross, ffn_gain, d_normed_ffn)
    d_after_cross = d_computed + d_cross_rows

    d_branch = pair_rows(d_after_cross.astype(bf16))
    d_mix = [mdot(d_branch, w).astype(bf16) for w in co]
    d_branch_cross = d_branch
    d_query, d_packed = attention_backward(
        cross_queries, d_mix, cross_mix, cross_packed, info, cross_lse, rows, CROSS_TILE, False
    )
    d_normed_cross = pair_sum(branch_out(d_query, cq), rows)
    d_encoder = (ndot(d_packed[0], cw[0]) + ndot(d_packed[1], cw[1])).astype(bf16)
    quarter = d_encoder.reshape((2, 2) + encoder_states.shape)
    kept = lax.dynamic_index_in_dim(quarter, chip, 0, keepdims=False)
    sent = lax.dynamic_index_in_dim(quarter, 1 - chip, 0, keepdims=False)
    kept = plus(kept, swap_ty(sent))
    mine = lax.dynamic_index_in_dim(kept, core, 0, keepdims=False)
    theirs = lax.dynamic_index_in_dim(kept, 1 - core, 0, keepdims=False)
    encoder_grad = mine.astype(f32) + swap_core(theirs).astype(f32)

    cross_parts = attention_grad(
        [
            (encoder, d_packed, (0, 768)),
            (normed_cross, d_query, (0, 256)),
            (d_branch_cross, cross_mix, (512, 768)),
        ]
    )
    d_self_rows, cross_gain_part = rms_backward(after_self, cross_gain, d_normed_cross)
    d_after_self = d_after_cross + d_self_rows

    d_branch = pair_rows(d_after_self.astype(bf16))
    d_mix = [mdot(d_branch, w).astype(bf16) for w in so]
    unused, d_packed = attention_backward(
        self_packed, d_mix, self_mix, self_packed, info, self_lse, rows, SELF_TILE, True
    )
    source_back = branch_out(d_packed, sw)
    d_before = pair_sum(source_back, rows).astype(bf16)
    d_later = lax.ppermute(d_before, "ty", [(1, 0)])

    def own_back(lo, hi):
        return source_back(2 * rows + lo, 2 * rows + hi)

    d_normed_self = pair_sum(own_back, rows) + d_later.astype(f32)
    self_parts = attention_grad(
        [(source, d_packed, (0, 768)), (d_branch, self_mix, (512, 768))]
    )
    d_chosen_rows, self_gain_part = rms_backward(chosen, self_gain, d_normed_self)
    d_chosen = d_after_self + d_chosen_rows
    first_grad = (
        predict[0, 0] * d_pred_first
        + predict[1, 0] * d_pred_second
        + jnp.where(picked, 0.0, d_chosen)
    )
    second_grad = (
        predict[0, 1] * d_pred_first
        + predict[1, 1] * d_pred_second
        + jnp.where(picked, d_chosen, 0.0)
    )
    input_grad = jnp.concatenate([first_grad, second_grad], axis=1)
    terms = (
        jnp.sum(d_pred_first * first_block),
        jnp.sum(d_pred_first * second_block),
        jnp.sum(d_pred_second * first_block),
        jnp.sum(d_pred_second * second_block),
        jnp.sum(d_first * gap),
        jnp.sum(d_second * gap),
    )
    row_at = lax.broadcasted_iota(jnp.int32, (8, half_width), 0)
    lane_at = lax.broadcasted_iota(jnp.int32, (8, half_width), 1)
    packed = jnp.where(row_at == 0, self_gain_part[None], 0.0)
    packed = jnp.where(row_at == 1, cross_gain_part[None], packed)
    packed = jnp.where(row_at == 2, ffn_gain_part[None], packed)
    for at, term in enumerate(terms):
        packed = jnp.where(jnp.logical_and(row_at == 3, lane_at == at), term, packed)
    (self_grads, cross_grads), packed = reduce_attention([self_parts, cross_parts], packed)

    def cut(grads):
        return tuple(grads[:, i * head_cols : (i + 1) * head_cols] for i in range(4))

    self_q_grad, self_k_grad, self_v_grad, self_o_grad = cut(self_grads)
    cross_q_grad, cross_k_grad, cross_v_grad, cross_o_grad = cut(cross_grads)
    return (
        widened_out,
        input_grad,
        encoder_grad,
        packed[3, :4].reshape(2, 2),
        packed[3, 4:6],
        packed[0],
        self_q_grad,
        self_k_grad,
        self_v_grad,
        self_o_grad,
        packed[1],
        cross_q_grad,
        cross_k_grad,
        cross_v_grad,
        cross_o_grad,
        packed[2],
        ffn_grads[:, :hidden_cols],
        ffn_grads[:, hidden_cols : 2 * hidden_cols],
        ffn_grads[:, 2 * hidden_cols :],
    )


def solution(mesh):
    dp, tensor = mesh.shape["dp"], mesh.shape["tensor"]
    split = Mesh(mesh.devices.reshape(dp, tensor // 2, 2), ("dp", "ty", "core"))
    tokens = P(("dp", "ty", "core"), None)
    weight = P("dp", ("ty", "core"))
    full = P()
    in_specs = (
        (tokens, tokens, full, full)
        + (full, weight, weight, weight, weight) * 2
        + (full, weight, weight, weight)
        + (P("dp", None), P("dp", None), P(("dp", "ty", "core")), tokens)
    )
    out_specs = (
        (tokens, tokens, tokens, full, full)
        + (full, weight, weight, weight, weight) * 2
        + (full, weight, weight, weight)
    )
    return jax.shard_map(body, mesh=split, in_specs=in_specs, out_specs=out_specs, check_vma=False)
```
